32 devices in a mesh: section: 4 (over y, x), mp: 8 (over z, core).
Axes of the slice: x: 2, y: 2, z: 4, core: 2. Of those that a mesh axis runs over, the one named last changes fastest.
Arguments:
- hidden_in: bfloat16 [1, 4, 64, 4096], P(None, 'section'), may hold values from -36 to 36
- attn_gain: bfloat16 [4, 4096], P('section'), may hold values from 0.5 to 2
- w_query: bfloat16 [4, 4096, 4096], P('section', None, 'mp'), may hold values from -0.75 to 0.75
- w_key: bfloat16 [4, 4096, 1024], P('section', None, 'mp'), may hold values from -0.0625 to 0.0625
- w_value: bfloat16 [4, 4096, 1024], P('section', None, 'mp'), may hold values from -0.09375 to 0.09375
- w_out: bfloat16 [4, 4096, 4096], P('section', 'mp'), may hold values from -0.09375 to 0.09375
- ffn_gain: bfloat16 [4, 4096], P('section'), may hold values from 0.5 to 2
- w_gate: bfloat16 [4, 4096, 14336], P('section', None, 'mp'), may hold values from -0.09375 to 0.09375
- w_up: bfloat16 [4, 4096, 14336], P('section', None, 'mp'), may hold values from -0.09375 to 0.09375
- w_down: bfloat16 [4, 14336, 4096], P('section', 'mp'), may hold values from -0.046875 to 0.046875
- ffn_blocks: int32 [4, 4], P(None, 'section'), may hold values from 1 to 112
- heads_on: int32 [4, 4], P(None, 'section'), may hold values from 1 to 32
Outputs:
- hidden_out: bfloat16 [1, 4, 64, 4096], P(None, 'section')
The draws below stay inside these ranges and needn't reach their ends.
Inputs may be any that keep to these rules, and one draw needn't show every extreme that they name: `ffn_blocks`: hidden units below 128 times the entry are active. `heads_on`: query heads below the entry are active.
All inputs are finite; a program needn't handle non-finite values.
Results may differ from the reference program's by a relative error of at most 0.025.
Values may be sent and summed in bfloat16 or wider, within the bound.
A program may use at most 128 MiB of HBM per device.

```python
import math
import jax
import jax.numpy as jnp
from jax import lax

D = 4096
HEADS = 32
KV_HEADS = 8
HD = 128
BLOCK = 128
FFB = 112
FF = 14336
FFP = 14336
SECTIONS = 4
LAYERS = 4
LEN = 64
MICRO_DEV = 1
MICRO = 4
N_MP = 8


def query_key_pair(key):
    folded = jax.random.fold_in(key, 7101)
    key_keys, key_query = jax.random.split(folded, 2)
    query_shape = (LAYERS, D, HEADS * HD)
    key_shape = (LAYERS, D, KV_HEADS * HD)
    spread_scale = D ** (-0.5)
    key_weight = jnp.clip(jax.random.normal(key_keys, key_shape, jnp.float32), -4.0, 4.0) * spread_scale
    query_weight = jnp.clip(jax.random.normal(key_query, query_shape, jnp.float32), -4.0, 4.0) * spread_scale
    return (query_weight, key_weight)


def draw_w_query(key, part):
    return query_key_pair(key)[0].astype(jnp.bfloat16)


def draw_w_key(key, part):
    return query_key_pair(key)[1].astype(jnp.bfloat16)


def draw_hidden_in(key, part):
    folded = jax.random.fold_in(key, 7202)
    key_noise, key_rows, key_columns = jax.random.split(folded, 3)
    array_shape = (MICRO_DEV, SECTIONS, LEN, D)
    low_end = jnp.log(0.3)
    high_end = jnp.log(3.0)
    row_scale = jnp.exp(jax.random.uniform(key_rows, (MICRO_DEV, SECTIONS, LEN, 1), jnp.float32, low_end, high_end))
    col_scale = jnp.exp(jax.random.uniform(key_columns, (1, 1, 1, D), jnp.float32, low_end, high_end))
    jitter = jnp.clip(jax.random.normal(key_noise, array_shape, jnp.float32), -4.0, 4.0)
    return (jitter * row_scale * col_scale).astype(jnp.bfloat16)


def place_ends(array, stream_key, least, high):
    index_at = [jax.random.randint(jax.random.fold_in(stream_key, axis), (), 0, length) for axis, length in enumerate(array.shape)]
    longest = array.shape.index(max(array.shape))
    next_to = index_at[:longest] + [(index_at[longest] + 1) % array.shape[longest]] + index_at[longest + 1:]
    return array.at[tuple(index_at)].set(least).at[tuple(next_to)].set(high)


def shard_levels(stream_key, shape, pieces, smallest, top_value):
    factor_of = 1.0
    for dim, shards_of in pieces:
        steps = jax.random.uniform(jax.random.fold_in(jax.random.fold_in(stream_key, 6), dim), (shards_of,), jnp.float32, smallest / len(pieces), top_value / len(pieces))
        factor_of = factor_of * jnp.repeat(jnp.exp(steps), shape[dim] // shards_of).reshape((-1,) + (1,) * (len(shape) - 1 - dim))
    return factor_of


def centred(key, extent, width, reach, pieces=(), held_as=jnp.bfloat16):
    factor_of = shard_levels(key, extent, pieces, -0.22, 0.18) if pieces else 1.0
    values = jax.random.normal(key, extent, jnp.float32) * width * factor_of
    return jnp.minimum(jnp.maximum(values, -reach), reach).astype(held_as)


def setup_inputs(seed: int = 0) -> dict:
    keys = jax.random.split(jax.random.key(seed), 13)
    hidden_in = draw_hidden_in(jax.random.fold_in(keys[12], 71), 0)
    attn_gain = jnp.clip(jnp.exp(math.log(2.0) - 1.3862944 * jax.random.uniform(keys[1], (LAYERS, D), jnp.float32) ** shard_levels(keys[1], (LAYERS, D), ((0, 4),), -0.2, 0.2)), 0.5, 2.0).astype(jnp.bfloat16)
    w_query = draw_w_query(jax.random.fold_in(keys[12], 71), 0)
    w_key = draw_w_key(jax.random.fold_in(keys[12], 71), 0)
    w_value = centred(keys[4], (LAYERS, D, KV_HEADS * HD), D ** -0.5, 0.09375, ((0, 4), (2, 8)))
    w_out = centred(keys[5], (LAYERS, HEADS * HD, D), (HEADS * HD) ** -0.5, 0.09375, ((0, 4), (1, 8)))
    ffn_gain = jnp.clip(jnp.exp(math.log(2.0) - 1.3862944 * jax.random.uniform(keys[6], (LAYERS, D), jnp.float32) ** shard_levels(keys[6], (LAYERS, D), ((0, 4),), -0.2, 0.2)), 0.5, 2.0).astype(jnp.bfloat16)
    w_gate = centred(keys[7], (LAYERS, D, FFP), D ** -0.5, 0.09375, ((0, 4), (2, 8)))
    w_up = centred(keys[8], (LAYERS, D, FFP), D ** -0.5, 0.09375, ((0, 4), (2, 8)))
    w_down = centred(keys[9], (LAYERS, FFP, D), FF ** -0.5, 0.046875, ((0, 4), (1, 8)))
    ffn_blocks = place_ends(jax.random.randint(keys[10], (MICRO, LAYERS), 1, FFB + 1), jax.random.fold_in(keys[10], 1), 1, FFB).astype(jnp.int32)
    heads_on = place_ends(jax.random.randint(keys[11], (MICRO, LAYERS), 1, HEADS + 1), jax.random.fold_in(keys[11], 1), 1, HEADS).astype(jnp.int32)
    return {"hidden_in": hidden_in, "attn_gain": attn_gain, "w_query": w_query, "w_key": w_key, "w_value": w_value, "w_out": w_out, "ffn_gain": ffn_gain, "w_gate": w_gate, "w_up": w_up, "w_down": w_down, "ffn_blocks": ffn_blocks, "heads_on": heads_on}


ROPE_BASE = 500000.0
EPSILON = 1e-05

def rms_scale(values, gain_row):
    mean_sq = lax.optimization_barrier(jnp.mean(values * values, axis=-1, keepdims=True))
    return values * lax.rsqrt(mean_sq + EPSILON) * gain_row.astype(jnp.float32)

def rotate(values):
    length = values.shape[0]
    half_dim = values.shape[-1] // 2
    frequency = ROPE_BASE ** (-(jnp.arange(half_dim, dtype=jnp.float32) / half_dim))
    angles = jnp.arange(length, dtype=jnp.float32)[:, None] * frequency[None, :]
    cosine_table = jnp.cos(angles)[:, None, :]
    sine_table = jnp.sin(angles)[:, None, :]
    front_half = values[..., :half_dim].astype(jnp.float32)
    back_half = values[..., half_dim:].astype(jnp.float32)
    return jnp.concatenate([front_half * cosine_table - back_half * sine_table, front_half * sine_table + back_half * cosine_table], axis=-1)

def group_sum(left, right):
    length, inner = left.shape
    group_width = inner // N_MP
    left_groups = left.reshape(length, N_MP, group_width).astype(jnp.float32)
    right_groups = right.reshape(N_MP, group_width, right.shape[1]).astype(jnp.float32)
    partials = jnp.einsum('tgk,gkd->gtd', left_groups, right_groups).astype(jnp.bfloat16)
    return lax.optimization_barrier(jnp.sum(partials.astype(jnp.float32), axis=0))

def layer_step(carried, layer_pos, active, block_count, attn_gain, w_query, w_key, w_value, w_out, ffn_gain, w_gate, w_up, w_down):
    length = carried.shape[0]
    group_size = HEADS // KV_HEADS
    residual = carried.astype(jnp.float32)
    normed = rms_scale(residual, attn_gain[layer_pos]).astype(jnp.bfloat16)
    queries = rotate(jnp.dot(normed, w_query[layer_pos], preferred_element_type=jnp.float32).reshape(length, HEADS, HD)).astype(jnp.bfloat16)
    key_proj = jnp.dot(normed, w_key[layer_pos], preferred_element_type=jnp.float32).astype(jnp.bfloat16).reshape(length, HD, KV_HEADS).transpose(0, 2, 1)
    keys_rot = rotate(key_proj).astype(jnp.bfloat16)
    values = jnp.dot(normed, w_value[layer_pos], preferred_element_type=jnp.float32).astype(jnp.bfloat16).reshape(length, HD, KV_HEADS).transpose(0, 2, 1)
    keys_all = jnp.repeat(keys_rot, group_size, axis=1)
    values_all = jnp.repeat(values, group_size, axis=1)
    scores = jnp.einsum('qhd,khd->hqk', queries.astype(jnp.float32), keys_all.astype(jnp.float32)) * HD ** (-0.5)
    causal = jnp.arange(length)[:, None] >= jnp.arange(length)[None, :]
    scores = jnp.where(causal[None], scores, -jnp.inf)
    probabilities = jax.nn.softmax(scores, axis=-1).astype(jnp.bfloat16)
    context = jnp.einsum('hqk,khd->qhd', probabilities.astype(jnp.float32), values_all.astype(jnp.float32))
    head_ids = jnp.arange(HEADS)
    context = jnp.where((head_ids < active)[None, :, None], context, 0.0).astype(jnp.bfloat16)
    attended = residual + group_sum(context.reshape(length, HEADS * HD), w_out[layer_pos])
    normed_ffn = rms_scale(attended, ffn_gain[layer_pos]).astype(jnp.bfloat16)
    gate_part = jnp.dot(normed_ffn, w_gate[layer_pos][:, :FF], preferred_element_type=jnp.float32)
    up_part = jnp.dot(normed_ffn, w_up[layer_pos][:, :FF], preferred_element_type=jnp.float32)
    unit_ids = jnp.arange(FF)
    hidden = jnp.where((unit_ids < BLOCK * block_count)[None, :], jax.nn.silu(gate_part) * up_part, 0.0).astype(jnp.bfloat16)
    padded = jnp.pad(hidden, ((0, 0), (0, w_gate.shape[2] - FF)))
    return (attended + group_sum(padded, w_down[layer_pos])).astype(jnp.bfloat16)

def reference(hidden_in, attn_gain, w_query, w_key, w_value, w_out, ffn_gain, w_gate, w_up, w_down, ffn_blocks, heads_on):
    finished = []
    for micro_index in range(MICRO):
        carried = hidden_in[micro_index // SECTIONS, micro_index % SECTIONS]
        for layer_pos in range(LAYERS):
            carried = layer_step(carried, layer_pos, heads_on[micro_index, layer_pos], ffn_blocks[micro_index, layer_pos], attn_gain, w_query, w_key, w_value, w_out, ffn_gain, w_gate, w_up, w_down)
        finished.append(carried)
    return jnp.stack(finished).reshape(MICRO_DEV, SECTIONS, LEN, D)
```

```python
import jax
import jax.numpy as jnp
import numpy as np
from jax import lax
from jax.experimental import pallas as pl
from jax.experimental.pallas import tpu as pltpu
from jax.sharding import PartitionSpec as P

HEADS = 32
KV_HEADS = 8
HD = 128
BLOCK = 128


ROPE_BASE = 500000.0
EPSILON = 1e-05


def passed_along(array, axis, by):
    peers = lax.axis_size(axis)
    return lax.ppermute(array, axis, [(i, (i + by) % peers) for i in range(peers)])


def rms_scale(values, gain_row):
    mean_sq = jnp.mean(values * values, axis=-1, keepdims=True)
    return values * lax.rsqrt(mean_sq + EPSILON) * gain_row.astype(jnp.float32)


def rotate(values):
    length = values.shape[0]
    half_dim = values.shape[-1] // 2
    frequency = ROPE_BASE ** (-(jnp.arange(half_dim, dtype=jnp.float32) / half_dim))
    angles = jnp.arange(length, dtype=jnp.float32)[:, None] * frequency[None, :]
    cosine_table = jnp.cos(angles)[:, None, :]
    sine_table = jnp.sin(angles)[:, None, :]
    front_half = values[..., :half_dim].astype(jnp.float32)
    back_half = values[..., half_dim:].astype(jnp.float32)
    return jnp.concatenate(
        [
            front_half * cosine_table - back_half * sine_table,
            front_half * sine_table + back_half * cosine_table,
        ],
        axis=-1,
    )


def attend_local(projected, query_width, key_width, active, first_head):
    length = projected.shape[0]
    heads_here = query_width // HD
    group_size = HEADS // KV_HEADS
    queries = rotate(projected[:, :query_width].reshape(length, heads_here, HD)).astype(
        jnp.bfloat16
    )
    key_local = projected[:, query_width : query_width + key_width].astype(jnp.bfloat16)
    value_local = projected[:, query_width + key_width :].astype(jnp.bfloat16)
    key_whole, value_whole = (
        lax.all_gather(key_local, "mp", axis=1, tiled=True),
        lax.all_gather(value_local, "mp", axis=1, tiled=True),
    )
    key_heads = key_whole.reshape(length, HD, KV_HEADS).transpose(0, 2, 1)
    value_heads = value_whole.reshape(length, HD, KV_HEADS).transpose(0, 2, 1)
    kv_here = max(1, heads_here // group_size)
    repeat_count = heads_here // kv_here
    first_kv = first_head // group_size
    key_pick = lax.dynamic_slice_in_dim(key_heads, first_kv, kv_here, 1)
    value_pick = lax.dynamic_slice_in_dim(value_heads, first_kv, kv_here, 1)
    keys_rot = jnp.repeat(rotate(key_pick).astype(jnp.bfloat16), repeat_count, axis=1)
    values = jnp.repeat(value_pick, repeat_count, axis=1)
    scores = jnp.einsum(
        "qhd,khd->hqk", queries, keys_rot, preferred_element_type=jnp.float32
    ) * HD ** (-0.5)
    causal = jnp.arange(length)[:, None] >= jnp.arange(length)[None, :]
    scores = jnp.where(causal[None], scores, -jnp.inf)
    probabilities = jax.nn.softmax(scores, axis=-1).astype(jnp.bfloat16)
    context = jnp.einsum("hqk,khd->qhd", probabilities, values, preferred_element_type=jnp.float32)
    head_ids = first_head + jnp.arange(heads_here)
    context = jnp.where((head_ids < active)[None, :, None], context, 0.0).astype(jnp.bfloat16)
    return context.reshape(length, query_width)


def per_device(
    hidden_in,
    attn_gain,
    w_query,
    w_key,
    w_value,
    w_out,
    ffn_gain,
    w_gate,
    w_up,
    w_down,
    ffn_blocks,
    heads_on,
):
    section_count = lax.axis_size("section")
    section_index = lax.axis_index("section")
    model_count = lax.axis_size("mp")
    model_index = lax.axis_index("mp")
    micro_total = ffn_blocks.shape[0]
    per_section = hidden_in.shape[0]
    length = hidden_in.shape[2]
    model_width = hidden_in.shape[3]
    local_rows = length // model_count
    units_here = w_gate.shape[2]
    query_width = w_query.shape[2]
    key_width = w_key.shape[2]
    first_head = model_index * (query_width // HD)
    first_unit = model_index * units_here
    joined_qkv = [jnp.concatenate([w_query[0], w_key[0], w_value[0]], axis=1)]
    joined_pair = [jnp.concatenate([w_gate[0], w_up[0]], axis=1)]

    def gated(pre_act, block_count):
        gate_part = pre_act[:, :units_here]
        up_part = pre_act[:, units_here:]
        unit_ids = first_unit + jnp.arange(units_here)
        return jnp.where(
            (unit_ids < BLOCK * block_count)[None, :], jax.nn.silu(gate_part) * up_part, 0.0
        ).astype(jnp.bfloat16)

    def layer_rows(carried, layer_pos, active, block_count):
        residual = carried.astype(jnp.float32)
        normed = rms_scale(residual, attn_gain[layer_pos]).astype(jnp.bfloat16)
        projected = jnp.dot(
            lax.all_gather(normed, "mp", axis=0, tiled=True),
            joined_qkv[layer_pos],
            preferred_element_type=jnp.float32,
        )
        context = attend_local(projected, query_width, key_width, active, first_head)
        attended = residual + lax.psum_scatter(
            jnp.dot(context, w_out[layer_pos], preferred_element_type=jnp.float32).astype(
                jnp.bfloat16
            ),
            "mp",
            scatter_dimension=0,
            tiled=True,
        ).astype(jnp.float32)
        normed_ffn = rms_scale(attended, ffn_gain[layer_pos]).astype(jnp.bfloat16)
        hidden = gated(
            jnp.dot(
                lax.all_gather(normed_ffn, "mp", axis=0, tiled=True),
                joined_pair[layer_pos],
                preferred_element_type=jnp.float32,
            ),
            block_count,
        )
        return (
            attended
            + lax.psum_scatter(
                jnp.dot(hidden, w_down[layer_pos], preferred_element_type=jnp.float32).astype(
                    jnp.bfloat16
                ),
                "mp",
                scatter_dimension=0,
                tiled=True,
            ).astype(jnp.float32)
        ).astype(jnp.bfloat16)

    def section_work(carried, moment, layer_fn):
        micro_index = jnp.clip(moment - section_index, 0, micro_total - 1)
        carried = layer_fn(carried, 0, heads_on[micro_index, 0], ffn_blocks[micro_index, 0])
        return carried

    def tick_step(moment, loop_carry):
        carried, slot_buffer = loop_carry
        cycle_index = moment // section_count
        incoming = lax.dynamic_index_in_dim(
            slot_buffer, jnp.minimum(cycle_index, per_section - 1), 0, keepdims=False
        )
        incoming = jnp.where(moment < micro_total, incoming, jnp.zeros_like(incoming))
        at_head = section_index == 0
        written = lax.dynamic_update_index_in_dim(
            slot_buffer, carried, jnp.maximum(cycle_index - 1, 0), 0
        )
        slot_buffer = jnp.where(at_head & (moment >= section_count), written, slot_buffer)
        carried = jnp.where(at_head, incoming, carried)
        carried = section_work(carried, moment, layer_rows)
        carried = passed_along(carried, "section", 1)
        slot_buffer = passed_along(slot_buffer, "section", -1)
        return (carried, slot_buffer)

    slot_start = hidden_in.reshape(per_section, length, model_width)
    slot_start = lax.dynamic_slice_in_dim(slot_start, model_index * local_rows, local_rows, 1)
    initial = jnp.zeros((local_rows, model_width), jnp.bfloat16)
    finished = lax.fori_loop(0, micro_total + section_count, tick_step, (initial, slot_start))
    result = finished[1]
    result = lax.all_gather(result, "mp", axis=1, tiled=True)
    return result.reshape(hidden_in.shape)


MESH = pl.DeviceIdType.MESH
BF16 = jnp.bfloat16
F32 = jnp.float32
TILE = 256


def tables(length):
    half = HD // 2
    frequency = np.float32(ROPE_BASE) ** (-(np.arange(half, dtype=np.float32) / np.float32(half)))
    angles = np.arange(length, dtype=np.float32)[:, None] * frequency[None, :].astype(np.float32)
    cosine, sine = np.cos(angles), np.sin(angles)
    q_cos = np.concatenate([cosine, cosine], axis=1)
    q_sin = np.concatenate([-sine, sine], axis=1)
    k_cos = np.concatenate([q_cos.T, np.ones((HD, length))], axis=1)
    k_sin = np.concatenate([q_sin.T, np.zeros((HD, length))], axis=1)
    return [jnp.asarray(t, F32) for t in (q_cos, q_sin, k_cos, k_sin)]


def remote(src, dst, send_sem, recv_sem, where):
    return pltpu.make_async_remote_copy(
        src_ref=src,
        dst_ref=dst,
        send_sem=send_sem,
        recv_sem=recv_sem,
        device_id=where,
        device_id_type=MESH,
    )


def layer_kernel(
    sections,
    peers,
    heads_hbm,
    blocks_hbm,
    hidden_in,
    attn_gain,
    ffn_gain,
    q_cos,
    q_sin,
    k_cos,
    k_sin,
    w_query,
    w_key,
    w_value,
    w_out,
    w_gate,
    w_up,
    w_down,
    out,
    v_query,
    v_kv,
    v_out,
    v_gate,
    v_up,
    v_down,
    heads_on,
    ffn_blocks,
    gains,
    x_in,
    x_ffn,
    final,
    scaled,
    squares,
    residual,
    query_buf,
    kv_send,
    kv_recv,
    context,
    acc_gate,
    acc_up,
    hidden,
    pair_send,
    pair_in,
    chip_send,
    chip_in,
    result,
    weight_sem,
    small_sem,
    stage_sem,
    seed_send,
    seed_recv,
    x_recv,
    x_relay_send,
    x_relay_recv,
    kv_send_sem,
    kv_recv_sem,
    pair_send_sem,
    pair_recv_sem,
    chip_send_sem,
    chip_recv_sem,
    ffn_mate_send,
    ffn_mate_recv,
    ffn_send,
    ffn_recv,
    ffn_relay_send,
    ffn_relay_recv,
    result_send,
    final_recv,
    final_relay_send,
    final_relay_recv,
    out_sem,
):
    sec = lax.axis_index("section")
    me = lax.axis_index("mp")
    chips = peers // 2
    chip, core = me // 2, me % 2
    mate_at = chip * 2 + 1 - core
    mate = (sec, mate_at)
    last = sections - 1
    length, block = x_in.shape[2:]
    width = peers * block
    heads_here = v_query.shape[1] // HD
    key_width = w_key.shape[1]
    units = v_gate.shape[1]
    high = chip // 2
    near = (chip, chip + 1 - 2 * (chip % 2), 2 - high, 3 * (1 - high))
    far = near[::-1]

    def nth(order, i):
        value = order[0]
        for k in range(1, len(order)):
            value = jnp.where(i == k, order[k], value)
        return value

    def offset(source, target):
        return (source - target + chips) % chips - 1

    def weight_copies():
        pairs = (
            (w_key, v_kv.at[:, pl.ds(0, key_width)]),
            (w_value, v_kv.at[:, pl.ds(key_width, key_width)]),
            (w_query, v_query),
            (w_out, v_out),
            (w_gate, v_gate),
            (w_up, v_up),
            (w_down, v_down),
        )
        return [
            pltpu.make_async_copy(a, b, weight_sem.at[i]) for i, (a, b) in enumerate(pairs)
        ]

    def columns(j):
        return pl.ds(pl.multiple_of(j * block, block), block)

    small = [
        pltpu.make_async_copy(heads_hbm, heads_on, small_sem.at[0]),
        pltpu.make_async_copy(blocks_hbm, ffn_blocks, small_sem.at[1]),
    ]
    for copy in small:
        copy.start()

    def staged(target):
        return [
            pltpu.make_async_copy(hidden_in.at[:, pl.ds(j * block, block)], target.at[j], stage_sem.at[j])
            for j in range(peers)
        ]

    @pl.when(sec == 0)
    def _():
        for copy in staged(x_in.at[0]):
            copy.start()

    @pl.when(sec != 0)
    def _():
        for copy in staged(final):
            copy.start()

    for copy in weight_copies():
        copy.start()

    barrier = pltpu.get_barrier_semaphore()
    for step in range(1, peers):
        pl.semaphore_signal(barrier, inc=1, device_id=(sec, (me + step) % peers), device_id_type=MESH)
    for step in range(1, sections):
        for away in range(chips):
            pl.semaphore_signal(
                barrier,
                inc=1,
                device_id=((sec + step) % sections, (chip + away) % chips * 2 + core),
                device_id_type=MESH,
            )
    pl.semaphore_wait(barrier, peers - 1 + (sections - 1) * chips)

    seed = remote(final, x_in.at[sec], seed_send, seed_recv.at[sec], (0, me))

    @pl.when(sec == 0)
    def _():
        for copy in staged(x_in.at[0]):
            copy.wait()

    @pl.when(sec != 0)
    def _():
        for copy in staged(final):
            copy.wait()
        seed.start()

    for row, gain in enumerate((attn_gain, ffn_gain)):
        for j in range(peers):
            gains[row, j] = jnp.broadcast_to(
                gain[:, j * block : (j + 1) * block].astype(F32), gains.shape[2:]
            )
    for copy in small:
        copy.wait()

    @pl.when(sec != 0)
    def _():
        seed.wait_send()

    def row_scale():
        total = jnp.sum(squares[...], axis=-1, keepdims=True)
        return lax.rsqrt(total * (1.0 / width) + EPSILON)

    def with_gain(row, j, values):
        x = values.astype(F32)
        part = x * x
        total = part[:, :HD]
        for k in range(1, block // HD):
            total = total + part[:, k * HD : (k + 1) * HD]
        squares[...] = squares[...] + total
        return (x * gains[row, j, 0:1, :]).astype(BF16)

    def x_direct(m, o, where):
        j = o * 2 + core
        return remote(x_in.at[m, j], x_in.at[m, j], result_send.at[m, o], x_recv.at[m, o], where)

    def x_relay(m, o):
        j = o * 2 + core
        return remote(x_in.at[m, j], x_in.at[m, j], x_relay_send.at[m, o], x_relay_recv.at[m, o], mate)

    def x_relayed(m, o):
        j = o * 2 + 1 - core
        return remote(x_in.at[m, j], x_in.at[m, j], x_relay_send.at[m, o], x_relay_recv.at[m, o], mate)

    def kv_copy(slot, step):
        to = (me + step) % peers
        return remote(
            kv_send.at[slot, to],
            kv_recv.at[slot, me],
            kv_send_sem.at[slot, step - 1],
            kv_recv_sem.at[slot, step - 1],
            (sec, to),
        )

    def pair_copy(slot, k):
        return remote(
            pair_send.at[slot, k], pair_in.at[slot, k], pair_send_sem.at[slot, k], pair_recv_sem.at[slot, k], mate
        )

    def chip_copy(slot, target):
        i = offset(chip, target)
        return remote(
            chip_send.at[slot, i],
            chip_in.at[slot, i],
            chip_send_sem.at[slot, i],
            chip_recv_sem.at[slot, i],
            (sec, target * 2 + core),
        )

    def ffn_mate(slot):
        return remote(
            x_ffn.at[slot, me], x_ffn.at[slot, me], ffn_mate_send.at[slot], ffn_mate_recv.at[slot], mate
        )

    def ffn_direct(slot, target):
        i = offset(chip, target)
        return remote(
            x_ffn.at[slot, me],
            x_ffn.at[slot, me],
            ffn_send.at[slot, i],
            ffn_recv.at[slot, i],
            (sec, target * 2 + core),
        )

    def ffn_arrival(slot, o):
        j = o * 2 + core
        i = offset(o, chip)
        return remote(x_ffn.at[slot, j], x_ffn.at[slot, j], ffn_send.at[slot, i], ffn_recv.at[slot, i], mate)

    def ffn_relay(slot, o, by):
        j = o * 2 + by
        i = offset(o, chip)
        return remote(
            x_ffn.at[slot, j], x_ffn.at[slot, j], ffn_relay_send.at[slot, i], ffn_relay_recv.at[slot, i], mate
        )

    def project(m):
        slot = m % 2
        squares[...] = jnp.zeros_like(squares)

        @pl.when((sec == 0) & (m != 0))
        def _():
            remote(x_in.at[m], x_in.at[m], seed_send, seed_recv.at[m], mate).wait_recv()

        def direct(i, _):
            o = nth(near, i)

            @pl.when(sec != 0)
            def _():
                x_direct(m, o, mate).wait_recv()
                x_relay(m, o).start()

            j = o * 2 + core
            scaled[:, columns(j)] = with_gain(0, j, x_in[m, j])
            return 0

        lax.fori_loop(0, chips, direct, 0)

        def relayed(i, _):
            o = nth(near, i)

            @pl.when(sec != 0)
            def _():
                x_relayed(m, o).wait_recv()

            j = o * 2 + 1 - core
            scaled[:, columns(j)] = with_gain(0, j, x_in[m, j])
            return 0

        lax.fori_loop(0, chips, relayed, 0)
        when_loaded(m, 0, 3)
        scale = row_scale()
        left = scaled[...]
        kv = (jnp.dot(left, v_kv[...], preferred_element_type=F32) * scale).astype(BF16)
        stacked = jnp.concatenate([kv[:, :key_width], kv[:, key_width:]], axis=0)
        r = lax.broadcasted_iota(jnp.int32, (key_width, key_width), 0)
        c = lax.broadcasted_iota(jnp.int32, (key_width, key_width), 1)
        parts_here = key_width // KV_HEADS
        pick = jnp.where(c == (r % parts_here) * KV_HEADS + r // parts_here, 1.0, 0.0).astype(BF16)
        by_head = lax.dot_general(
            pick, stacked, (((1,), (1,)), ((), ())), preferred_element_type=F32
        )
        kv_send[slot] = by_head.astype(BF16).reshape(KV_HEADS, parts_here, 2 * length)
        for step in range(1, peers):
            kv_copy(slot, step).start()
        kv_recv[slot, me] = kv_send[slot, me]
        query = jnp.dot(left, v_query[...], preferred_element_type=F32) * scale
        for h in range(heads_here):
            head = query[:, h * HD : (h + 1) * HD]
            query_buf[slot, pl.ds(h * length, length), :] = (
                head * q_cos[...] + pltpu.roll(head, HD // 2, 1) * q_sin[...]
            ).astype(BF16)

    def attend(m):
        slot = m % 2
        for step in range(1, peers):
            kv_copy(slot, step).wait()
        pair = kv_recv[slot].reshape(HD, 2 * length).astype(F32)
        swapped = jnp.concatenate([pair[HD // 2 :], pair[: HD // 2]], axis=0)
        pair = (pair * k_cos[...] + swapped * k_sin[...]).astype(BF16)
        scores = jnp.dot(query_buf[slot], pair, preferred_element_type=F32) * HD ** (-0.5)
        token = lax.broadcasted_iota(jnp.int32, scores.shape, 0) % length
        key_at = lax.broadcasted_iota(jnp.int32, scores.shape, 1)
        scores = jnp.where(key_at <= token, scores, -jnp.inf)
        scores = jnp.exp(scores - jnp.max(scores, axis=-1, keepdims=True))
        chances = scores / jnp.sum(scores, axis=-1, keepdims=True)
        chances = pltpu.roll(chances, length, 1).astype(BF16)
        mixed = lax.dot_general(
            chances, pair, (((1,), (1,)), ((), ())), preferred_element_type=F32
        )
        for h in range(heads_here):
            on = me * heads_here + h < heads_on[m, 0]
            rows = mixed[h * length : (h + 1) * length]
            context[:, h * HD : (h + 1) * HD] = jnp.where(on, rows, 0.0).astype(BF16)
        when_loaded(m, 3, 4)
        scatter(slot, context, v_out, x_in[m, me].astype(F32))

    def scatter(slot, left, weight, base):
        def to_mate(k, _):
            at = columns(nth(far, k) * 2 + 1 - core)
            pair_send[slot, k] = jnp.dot(left[...], weight[:, at], preferred_element_type=F32).astype(BF16)
            pair_copy(slot, k).start()
            return 0

        lax.fori_loop(0, chips, to_mate, 0)

        def to_chip(k, _):
            target = nth(far, k)
            term = jnp.dot(left[...], weight[:, columns(target * 2 + core)], preferred_element_type=F32)
            pair_copy(slot, k).wait_recv()
            i = offset(chip, target)
            chip_send[slot, i] = (term + pair_in[slot, k].astype(F32)).astype(BF16)
            chip_copy(slot, target).start()
            return 0

        lax.fori_loop(0, chips - 1, to_chip, 0)
        term = jnp.dot(left[...], weight[:, columns(me)], preferred_element_type=F32)
        residual[slot] = base + term

    def gathered_sum(slot):
        for k in range(chips):
            pair_copy(slot, k).wait_send()
        pair_copy(slot, chips - 1).wait_recv()
        total = residual[slot] + pair_in[slot, chips - 1].astype(F32)
        for k in range(chips - 1):
            pltpu.make_async_copy(chip_in.at[slot, k], chip_in.at[slot, k], chip_recv_sem.at[slot, k]).wait()
            total = total + chip_in[slot, k].astype(F32)
            pltpu.make_async_copy(chip_send.at[slot, k], chip_send.at[slot, k], chip_send_sem.at[slot, k]).wait()
        return total

    def share(m):
        slot = m % 2
        attended = gathered_sum(slot)
        residual[slot] = attended
        x_ffn[slot, me] = attended.astype(BF16)
        for o in near[1:]:
            ffn_direct(slot, o).start()
        ffn_mate(slot).start()

    def feed_forward(m):
        slot = m % 2
        when_loaded(m, 4, 6)
        squares[...] = jnp.zeros_like(squares)

        def piece(j, first):
            left = with_gain(1, j, x_ffn[slot, j])
            rows = columns(j)
            for weight, acc in ((v_gate, acc_gate), (v_up, acc_up)):
                term = jnp.dot(left, weight[rows, :], preferred_element_type=F32)
                acc[...] = term if first else acc[...] + term

        piece(me, True)
        ffn_mate(slot).wait_recv()
        piece(mate_at, False)

        def from_chip(i, _):
            o = nth(near, i)
            ffn_arrival(slot, o).wait_recv()
            ffn_relay(slot, o, core).start()
            piece(o * 2 + core, False)
            ffn_relay(slot, o, 1 - core).wait_recv()
            piece(o * 2 + 1 - core, False)
            return 0

        lax.fori_loop(1, chips, from_chip, 0)
        scale = row_scale()
        active = BLOCK * ffn_blocks[m, 0]

        def activate(i, _):
            at = pl.ds(pl.multiple_of(i * TILE, TILE), TILE)
            gate = acc_gate[:, at] * scale
            up = acc_up[:, at] * scale
            unit = me * units + i * TILE + lax.broadcasted_iota(jnp.int32, gate.shape, 1)
            value = gate / (1.0 + jnp.exp(-gate)) * up
            hidden[:, at] = jnp.where(unit < active, value, 0.0).astype(BF16)
            return 0

        lax.fori_loop(0, units // TILE, activate, 0)
        when_loaded(m, 6, 7)
        scatter(slot, hidden, v_down, residual[slot])
        ffn_mate(slot).wait_send()
        for o in near[1:]:
            ffn_direct(slot, o).wait_send()
            ffn_relay(slot, o, core).wait_send()

    def hand_over(m):
        result[m] = gathered_sum(m % 2).astype(BF16)
        for o in near:
            here = (sec == last) & (m == last) & (o == chip)

            @pl.when(sec < last)
            def _():
                remote(
                    result.at[m], x_in.at[m, me], result_send.at[m, o], x_recv.at[m, chip], (sec + 1, o * 2 + core)
                ).start()

            if o is not chip:

                @pl.when(sec == last)
                def _():
                    remote(
                        result.at[m], final.at[me], result_send.at[m, o], final_recv.at[chip], (m, o * 2 + core)
                    ).start()

        @pl.when((sec == last) & (m != last))
        def _():
            remote(
                result.at[m], final.at[me], result_send.at[m, chip], final_recv.at[chip], (m, me)
            ).start()

        @pl.when((sec == last) & (m == last))
        def _():
            pltpu.make_async_copy(result.at[m], final.at[me], final_recv.at[chip]).start()

    def when_loaded(m, first, stop):
        @pl.when(m == 0)
        def _():
            for copy in weight_copies()[first:stop]:
                copy.wait()

    def micro_step(m, _):
        project(m)
        attend(m)

        @pl.when(m > 0)
        def _():
            hand_over(m - 1)

        share(m)
        feed_forward(m)
        return 0

    lax.fori_loop(0, sections, micro_step, 0)
    hand_over(last)

    def drain(m, _):
        for o in range(chips):

            @pl.when((sec < last) | (m < last) | (o != chip))
            def _():
                remote(result.at[m], final.at[me], result_send.at[m, o], final_recv.at[chip], mate).wait_send()

            @pl.when(sec != 0)
            def _():
                x_relay(m, o).wait_send()

        return 0

    lax.fori_loop(0, sections, drain, 0)

    def final_copy(o, by):
        j = o * 2 + by
        return remote(final.at[j], final.at[j], final_relay_send.at[o], final_relay_recv.at[o], mate)

    def to_output(j):
        return pltpu.make_async_copy(final.at[j], out.at[:, columns(j)], out_sem.at[j])

    for o in near:
        j = o * 2 + core
        remote(final.at[j], final.at[j], result_send.at[0, o], final_recv.at[o], mate).wait_recv()
        final_copy(o, core).start()
        to_output(j).start()
    for o in near:
        final_copy(o, 1 - core).wait_recv()
        to_output(o * 2 + 1 - core).start()
    for o in near:
        final_copy(o, core).wait_send()
    for j in range(peers):
        to_output(j).wait()


def resident(hidden_in, attn_gain, w_query, w_key, w_value, w_out, ffn_gain, w_gate, w_up, w_down, ffn_blocks, heads_on):
    sections, peers = lax.axis_size("section"), lax.axis_size("mp")
    length, width = hidden_in.shape[2:]
    block, chips = width // peers, peers // 2
    units, key_width = w_gate.shape[2], w_key.shape[2]
    query_width = w_query.shape[2]
    parts_here = key_width // KV_HEADS
    vmem = pl.BlockSpec(memory_space=pltpu.VMEM)
    hbm = pl.BlockSpec(memory_space=pl.ANY)
    dma = pltpu.SemaphoreType.DMA
    half = pltpu.VMEM
    result = pl.pallas_call(
        lambda *refs: layer_kernel(sections, peers, *refs),
        out_shape=jax.ShapeDtypeStruct((length, width), BF16),
        in_specs=[hbm] * 3 + [vmem] * 6 + [hbm] * 7,
        out_specs=hbm,
        scratch_shapes=[
            half((width, query_width), BF16),
            half((width, 2 * key_width), BF16),
            half((query_width, width), BF16),
            half((width, units), BF16),
            half((width, units), BF16),
            half((units, width), BF16),
            pltpu.SMEM(heads_on.shape, jnp.int32),
            pltpu.SMEM(ffn_blocks.shape, jnp.int32),
            half((2, peers, 8, block), F32),
            half((sections, peers, length, block), BF16),
            half((2, peers, length, block), BF16),
            half((peers, length, block), BF16),
            half((length, width), BF16),
            half((length, HD), F32),
            half((2, length, block), F32),
            half((2, query_width // HD * length, HD), BF16),
            half((2, peers, parts_here, 2 * length), BF16),
            half((2, peers, parts_here, 2 * length), BF16),
            half((length, query_width), BF16),
            half((length, units), F32),
            half((length, units), F32),
            half((length, units), BF16),
            half((2, chips, length, block), BF16),
            half((2, chips, length, block), BF16),
            half((2, chips - 1, length, block), BF16),
            half((2, chips - 1, length, block), BF16),
            half((sections, length, block), BF16),
            dma((7,)),
            dma((2,)),
            dma((peers,)),
            dma,
            dma((sections,)),
            dma((sections, chips)),
            dma((sections, chips)),
            dma((sections, chips)),
            dma((2, peers - 1)),
            dma((2, peers - 1)),
            dma((2, chips)),
            dma((2, chips)),
            dma((2, chips - 1)),
            dma((2, chips - 1)),
            dma((2,)),
            dma((2,)),
            dma((2, chips - 1)),
            dma((2, chips - 1)),
            dma((2, chips - 1)),
            dma((2, chips - 1)),
            dma((sections, chips)),
            dma((chips,)),
            dma((chips,)),
            dma((chips,)),
            dma((peers,)),
        ],
        compiler_params=pltpu.CompilerParams(
            collective_id=0, has_side_effects=True, vmem_limit_bytes=67043328
        ),
    )(
        heads_on,
        ffn_blocks,
        hidden_in.reshape(length, width),
        attn_gain,
        ffn_gain,
        *tables(length),
        w_query[0],
        w_key[0],
        w_value[0],
        w_out[0],
        w_gate[0],
        w_up[0],
        w_down[0],
    )
    return result.reshape(hidden_in.shape)


def one_device(*args):
    hidden_in, w_query, w_key, w_gate = args[0], args[2], args[3], args[7]
    sections, peers = lax.axis_size("section"), lax.axis_size("mp")
    fits = (
        hidden_in.shape[0] == 1
        and args[10].shape[0] == sections
        and peers == KV_HEADS
        and sections == 4
        and args[5].shape[1] == w_query.shape[2]
        and 2 * hidden_in.shape[2] == HD
        and w_query.shape[2] * KV_HEADS == HEADS * HD
        and w_key.shape[2] == HD
        and w_gate.shape[2] % TILE == 0
        and hidden_in.shape[3] % (peers * HD) == 0
        and hidden_in.shape[3] == HEADS * HD
    )
    return (resident if fits else per_device)(*args)


def solution(mesh):
    return jax.shard_map(
        one_device,
        mesh=mesh,
        in_specs=(
            P(None, "section", None, None),
            P("section", None),
            P("section", None, "mp"),
            P("section", None, "mp"),
            P("section", None, "mp"),
            P("section", "mp", None),
            P("section", None),
            P("section", None, "mp"),
            P("section", None, "mp"),
            P("section", "mp", None),
            P(None, "section"),
            P(None, "section"),
        ),
        out_specs=P(None, "section", None, None),
        check_vma=False,
    )
```

```python
import jax
import jax.numpy as jnp
import numpy as np
from jax import lax
from jax.experimental import pallas as pl
from jax.experimental.pallas import tpu as pltpu
from jax.sharding import PartitionSpec as P

HEADS = 32
KV_HEADS = 8
HD = 128
BLOCK = 128


ROPE_BASE = 500000.0
EPSILON = 1e-05


def passed_along(array, axis, by):
    peers = lax.axis_size(axis)
    return lax.ppermute(array, axis, [(i, (i + by) % peers) for i in range(peers)])


def rms_scale(values, gain_row):
    mean_sq = jnp.mean(values * values, axis=-1, keepdims=True)
    return values * lax.rsqrt(mean_sq + EPSILON) * gain_row.astype(jnp.float32)


def rotate(values):
    length = values.shape[0]
    half_dim = values.shape[-1] // 2
    frequency = ROPE_BASE ** (-(jnp.arange(half_dim, dtype=jnp.float32) / half_dim))
    angles = jnp.arange(length, dtype=jnp.float32)[:, None] * frequency[None, :]
    cosine_table = jnp.cos(angles)[:, None, :]
    sine_table = jnp.sin(angles)[:, None, :]
    front_half = values[..., :half_dim].astype(jnp.float32)
    back_half = values[..., half_dim:].astype(jnp.float32)
    return jnp.concatenate(
        [
            front_half * cosine_table - back_half * sine_table,
            front_half * sine_table + back_half * cosine_table,
        ],
        axis=-1,
    )


def attend_local(projected, query_width, key_width, active, first_head):
    length = projected.shape[0]
    heads_here = query_width // HD
    group_size = HEADS // KV_HEADS
    queries = rotate(projected[:, :query_width].reshape(length, heads_here, HD)).astype(
        jnp.bfloat16
    )
    key_local = projected[:, query_width : query_width + key_width].astype(jnp.bfloat16)
    value_local = projected[:, query_width + key_width :].astype(jnp.bfloat16)
    key_whole, value_whole = (
        lax.all_gather(key_local, "mp", axis=1, tiled=True),
        lax.all_gather(value_local, "mp", axis=1, tiled=True),
    )
    key_heads = key_whole.reshape(length, HD, KV_HEADS).transpose(0, 2, 1)
    value_heads = value_whole.reshape(length, HD, KV_HEADS).transpose(0, 2, 1)
    kv_here = max(1, heads_here // group_size)
    repeat_count = heads_here // kv_here
    first_kv = first_head // group_size
    key_pick = lax.dynamic_slice_in_dim(key_heads, first_kv, kv_here, 1)
    value_pick = lax.dynamic_slice_in_dim(value_heads, first_kv, kv_here, 1)
    keys_rot = jnp.repeat(rotate(key_pick).astype(jnp.bfloat16), repeat_count, axis=1)
    values = jnp.repeat(value_pick, repeat_count, axis=1)
    scores = jnp.einsum(
        "qhd,khd->hqk", queries, keys_rot, preferred_element_type=jnp.float32
    ) * HD ** (-0.5)
    causal = jnp.arange(length)[:, None] >= jnp.arange(length)[None, :]
    scores = jnp.where(causal[None], scores, -jnp.inf)
    probabilities = jax.nn.softmax(scores, axis=-1).astype(jnp.bfloat16)
    context = jnp.einsum("hqk,khd->qhd", probabilities, values, preferred_element_type=jnp.float32)
    head_ids = first_head + jnp.arange(heads_here)
    context = jnp.where((head_ids < active)[None, :, None], context, 0.0).astype(jnp.bfloat16)
    return context.reshape(length, query_width)


def per_device(
    hidden_in,
    attn_gain,
    w_query,
    w_key,
    w_value,
    w_out,
    ffn_gain,
    w_gate,
    w_up,
    w_down,
    ffn_blocks,
    heads_on,
):
    section_count = lax.axis_size("section")
    section_index = lax.axis_index("section")
    model_count = lax.axis_size("mp")
    model_index = lax.axis_index("mp")
    micro_total = ffn_blocks.shape[0]
    per_section = hidden_in.shape[0]
    length = hidden_in.shape[2]
    model_width = hidden_in.shape[3]
    local_rows = length // model_count
    units_here = w_gate.shape[2]
    query_width = w_query.shape[2]
    key_width = w_key.shape[2]
    first_head = model_index * (query_width // HD)
    first_unit = model_index * units_here
    joined_qkv = [jnp.concatenate([w_query[0], w_key[0], w_value[0]], axis=1)]
    joined_pair = [jnp.concatenate([w_gate[0], w_up[0]], axis=1)]

    def gated(pre_act, block_count):
        gate_part = pre_act[:, :units_here]
        up_part = pre_act[:, units_here:]
        unit_ids = first_unit + jnp.arange(units_here)
        return jnp.where(
            (unit_ids < BLOCK * block_count)[None, :], jax.nn.silu(gate_part) * up_part, 0.0
        ).astype(jnp.bfloat16)

    def layer_rows(carried, layer_pos, active, block_count):
        residual = carried.astype(jnp.float32)
        normed = rms_scale(residual, attn_gain[layer_pos]).astype(jnp.bfloat16)
        projected = jnp.dot(
            lax.all_gather(normed, "mp", axis=0, tiled=True),
            joined_qkv[layer_pos],
            preferred_element_type=jnp.float32,
        )
        context = attend_local(projected, query_width, key_width, active, first_head)
        attended = residual + lax.psum_scatter(
            jnp.dot(context, w_out[layer_pos], preferred_element_type=jnp.float32).astype(
                jnp.bfloat16
            ),
            "mp",
            scatter_dimension=0,
            tiled=True,
        ).astype(jnp.float32)
        normed_ffn = rms_scale(attended, ffn_gain[layer_pos]).astype(jnp.bfloat16)
        hidden = gated(
            jnp.dot(
                lax.all_gather(normed_ffn, "mp", axis=0, tiled=True),
                joined_pair[layer_pos],
                preferred_element_type=jnp.float32,
            ),
            block_count,
        )
        return (
            attended
            + lax.psum_scatter(
                jnp.dot(hidden, w_down[layer_pos], preferred_element_type=jnp.float32).astype(
                    jnp.bfloat16
                ),
                "mp",
                scatter_dimension=0,
                tiled=True,
            ).astype(jnp.float32)
        ).astype(jnp.bfloat16)

    def section_work(carried, moment, layer_fn):
        micro_index = jnp.clip(moment - section_index, 0, micro_total - 1)
        carried = layer_fn(carried, 0, heads_on[micro_index, 0], ffn_blocks[micro_index, 0])
        return carried

    def tick_step(moment, loop_carry):
        carried, slot_buffer = loop_carry
        cycle_index = moment // section_count
        incoming = lax.dynamic_index_in_dim(
            slot_buffer, jnp.minimum(cycle_index, per_section - 1), 0, keepdims=False
        )
        incoming = jnp.where(moment < micro_total, incoming, jnp.zeros_like(incoming))
        at_head = section_index == 0
        written = lax.dynamic_update_index_in_dim(
            slot_buffer, carried, jnp.maximum(cycle_index - 1, 0), 0
        )
        slot_buffer = jnp.where(at_head & (moment >= section_count), written, slot_buffer)
        carried = jnp.where(at_head, incoming, carried)
        carried = section_work(carried, moment, layer_rows)
        carried = passed_along(carried, "section", 1)
        slot_buffer = passed_along(slot_buffer, "section", -1)
        return (carried, slot_buffer)

    slot_start = hidden_in.reshape(per_section, length, model_width)
    slot_start = lax.dynamic_slice_in_dim(slot_start, model_index * local_rows, local_rows, 1)
    initial = jnp.zeros((local_rows, model_width), jnp.bfloat16)
    finished = lax.fori_loop(0, micro_total + section_count, tick_step, (initial, slot_start))
    result = finished[1]
    result = lax.all_gather(result, "mp", axis=1, tiled=True)
    return result.reshape(hidden_in.shape)


MESH = pl.DeviceIdType.MESH
BF16 = jnp.bfloat16
F32 = jnp.float32
TILE = 256


def tables(length):
    half = HD // 2
    frequency = np.float32(ROPE_BASE) ** (-(np.arange(half, dtype=np.float32) / np.float32(half)))
    angles = np.arange(length, dtype=np.float32)[:, None] * frequency[None, :].astype(np.float32)
    cosine, sine = np.cos(angles), np.sin(angles)
    q_cos = np.concatenate([cosine, cosine], axis=1)
    q_sin = np.concatenate([-sine, sine], axis=1)
    k_cos = np.concatenate([q_cos.T, np.ones((HD, length))], axis=1)
    k_sin = np.concatenate([q_sin.T, np.zeros((HD, length))], axis=1)
    return [jnp.asarray(t, F32) for t in (q_cos, q_sin, k_cos, k_sin)]


def remote(src, dst, send_sem, recv_sem, where):
    return pltpu.make_async_remote_copy(
        src_ref=src,
        dst_ref=dst,
        send_sem=send_sem,
        recv_sem=recv_sem,
        device_id=where,
        device_id_type=MESH,
    )


def layer_kernel(
    sections,
    peers,
    heads_hbm,
    blocks_hbm,
    hidden_in,
    attn_gain,
    ffn_gain,
    q_cos,
    q_sin,
    k_cos,
    k_sin,
    w_query,
    w_key,
    w_value,
    w_out,
    w_gate,
    w_up,
    w_down,
    out,
    v_query,
    v_kv,
    v_out,
    v_gate,
    v_up,
    v_down,
    heads_on,
    ffn_blocks,
    gains,
    x_in,
    x_ffn,
    final,
    scaled,
    squares,
    residual,
    query_buf,
    key_buf,
    value_buf,
    mixed_buf,
    kv_send,
    kv_recv,
    context,
    acc_gate,
    acc_up,
    hidden,
    pair_send,
    pair_in,
    chip_send,
    chip_in,
    result,
    weight_sem,
    head_send_sem,
    head_recv_sem,
    small_sem,
    stage_sem,
    seed_send,
    seed_recv,
    x_recv,
    x_relay_send,
    x_relay_recv,
    kv_send_sem,
    kv_recv_sem,
    pair_send_sem,
    pair_recv_sem,
    chip_send_sem,
    chip_recv_sem,
    ffn_mate_send,
    ffn_mate_recv,
    ffn_send,
    ffn_recv,
    ffn_relay_send,
    ffn_relay_recv,
    result_send,
    final_recv,
    final_relay_send,
    final_relay_recv,
    out_sem,
):
    sec = lax.axis_index("section")
    me = lax.axis_index("mp")
    chips = peers // 2
    chip, core = me // 2, me % 2
    mate_at = chip * 2 + 1 - core
    mate = (sec, mate_at)
    last = sections - 1
    length, block = x_in.shape[2:]
    width = peers * block
    heads_here = v_query.shape[1] // HD
    key_width = w_key.shape[1]
    units = v_gate.shape[1]
    high = chip // 2
    near = (chip, chip + 1 - 2 * (chip % 2), 2 - high, 3 * (1 - high))
    far = near[::-1]

    def nth(order, i):
        value = order[0]
        for k in range(1, len(order)):
            value = jnp.where(i == k, order[k], value)
        return value

    def offset(source, target):
        return (source - target + chips) % chips - 1

    def weight_copies():
        pairs = (
            (w_key, v_kv.at[:, pl.ds(0, key_width)]),
            (w_value, v_kv.at[:, pl.ds(key_width, key_width)]),
            (w_query, v_query),
            (w_out, v_out),
            (w_gate, v_gate),
            (w_up, v_up),
            (w_down, v_down),
        )
        return [
            pltpu.make_async_copy(a, b, weight_sem.at[i]) for i, (a, b) in enumerate(pairs)
        ]

    def columns(j):
        return pl.ds(pl.multiple_of(j * block, block), block)

    small = [
        pltpu.make_async_copy(heads_hbm, heads_on, small_sem.at[0]),
        pltpu.make_async_copy(blocks_hbm, ffn_blocks, small_sem.at[1]),
    ]
    for copy in small:
        copy.start()

    def staged(target):
        return [
            pltpu.make_async_copy(hidden_in.at[:, pl.ds(j * block, block)], target.at[j], stage_sem.at[j])
            for j in range(peers)
        ]

    @pl.when(sec == 0)
    def _():
        for copy in staged(x_in.at[0]):
            copy.start()

    @pl.when(sec != 0)
    def _():
        for copy in staged(final):
            copy.start()

    for copy in weight_copies()[:2]:
        copy.start()

    @pl.when(sec == 0)
    def _():
        for copy in weight_copies()[2:]:
            copy.start()

    barrier = pltpu.get_barrier_semaphore()
    for step in range(1, peers):
        pl.semaphore_signal(barrier, inc=1, device_id=(sec, (me + step) % peers), device_id_type=MESH)
    for step in range(1, sections):
        for away in range(chips):
            pl.semaphore_signal(
                barrier,
                inc=1,
                device_id=((sec + step) % sections, (chip + away) % chips * 2 + core),
                device_id_type=MESH,
            )
    pl.semaphore_wait(barrier, peers - 1 + (sections - 1) * chips)

    seed = remote(final, x_in.at[sec], seed_send, seed_recv.at[sec], (0, me))

    @pl.when(sec == 0)
    def _():
        for copy in staged(x_in.at[0]):
            copy.wait()

    @pl.when(sec != 0)
    def _():
        for copy in staged(final):
            copy.wait()
        seed.start()

    for row, gain in enumerate((attn_gain, ffn_gain)):
        for j in range(peers):
            gains[row, j] = jnp.broadcast_to(
                gain[:, j * block : (j + 1) * block].astype(F32), gains.shape[2:]
            )
    for copy in small:
        copy.wait()

    parts_here = key_width // KV_HEADS
    tile_row = lax.broadcasted_iota(jnp.int32, (key_width, key_width), 0)
    tile_col = lax.broadcasted_iota(jnp.int32, (key_width, key_width), 1)
    by_heads = tile_col == tile_row % parts_here * KV_HEADS + tile_row // parts_here
    pick = jnp.where(by_heads, 1.0, 0.0).astype(BF16)
    same = jnp.where(tile_col == tile_row, 1.0, 0.0).astype(BF16)

    def head_rows(which, by, received):
        at = received * 2 * key_width + which * key_width + by * parts_here
        return v_down.at[pl.ds(pl.multiple_of(at, parts_here), parts_here), :]

    def head_copy(which, k, b):
        to = far[k] * 2 + (1 - core if b else core)
        i = offset(chip, far[k]) * 2 + b if k < chips - 1 else peers - 2
        return remote(
            head_rows(which, to, 0),
            head_rows(which, me, 1),
            head_send_sem.at[which, i],
            head_recv_sem.at[which, i],
            (sec, to),
        )

    def head_arrival(which, k, b):
        by = far[k] * 2 + (1 - core if b else core)
        i = offset(far[k], chip) * 2 + b if k < chips - 1 else peers - 2
        there = head_rows(which, by, 1)
        return remote(there, there, head_send_sem.at[which, i], head_recv_sem.at[which, i], mate)

    head_order = [(k, b) for k in range(chips - 1) for b in range(2)] + [(chips - 1, 1)]

    def stripe(i):
        return pl.ds(pl.multiple_of(i * block, block), block)

    @pl.when(sec != 0)
    def _():
        seed.wait_send()
        for copy in weight_copies()[:2]:
            copy.wait()

        for which in range(2):
            rows = pl.ds(which * key_width, key_width)

            def to_heads(i, _):
                turned = lax.dot_general(
                    pick, v_kv[stripe(i), rows], (((1,), (1,)), ((), ())), preferred_element_type=F32
                )
                v_down[rows, stripe(i)] = turned.astype(BF16)
                return 0

            lax.fori_loop(0, peers, to_heads, 0)
            for k, b in head_order:
                head_copy(which, k, b).start()
            own = pl.multiple_of(which * key_width + me * parts_here, parts_here)
            v_down[pl.ds(2 * key_width + own, parts_here), :] = v_down[pl.ds(own, parts_here), :]
        for copy in weight_copies()[2:-1]:
            copy.start()
        for which in range(2):
            for k, b in head_order:
                head_copy(which, k, b).wait_send()
                head_arrival(which, k, b).wait_recv()
            rows = pl.ds(which * key_width, key_width)

            def from_heads(i, _):
                turned = lax.dot_general(
                    v_down[pl.ds((2 + which) * key_width, key_width), stripe(i)],
                    same,
                    (((0,), (0,)), ((), ())),
                    preferred_element_type=F32,
                )
                v_kv[stripe(i), rows] = turned.astype(BF16)
                return 0

            lax.fori_loop(0, peers, from_heads, 0)
        weight_copies()[-1].start()

    def row_scale():
        total = jnp.sum(squares[...], axis=-1, keepdims=True)
        return lax.rsqrt(total * (1.0 / width) + EPSILON)

    def with_gain(row, j, values):
        x = values.astype(F32)
        part = x * x
        total = part[:, :HD]
        for k in range(1, block // HD):
            total = total + part[:, k * HD : (k + 1) * HD]
        squares[...] = squares[...] + total
        return (x * gains[row, j, 0:1, :]).astype(BF16)

    def x_direct(m, o, where):
        j = o * 2 + core
        return remote(x_in.at[m, j], x_in.at[m, j], result_send.at[m, o], x_recv.at[m, o], where)

    def x_relay(m, o):
        j = o * 2 + core
        return remote(x_in.at[m, j], x_in.at[m, j], x_relay_send.at[m, o], x_relay_recv.at[m, o], mate)

    def x_relayed(m, o):
        j = o * 2 + 1 - core
        return remote(x_in.at[m, j], x_in.at[m, j], x_relay_send.at[m, o], x_relay_recv.at[m, o], mate)

    def kv_copy(slot, step):
        to = (me + step) % peers
        return remote(
            kv_send.at[slot, to],
            kv_recv.at[slot, me],
            kv_send_sem.at[slot, step - 1],
            kv_recv_sem.at[slot, step - 1],
            (sec, to),
        )

    def pair_copy(slot, k):
        return remote(
            pair_send.at[slot, k], pair_in.at[slot, k], pair_send_sem.at[slot, k], pair_recv_sem.at[slot, k], mate
        )

    def chip_copy(slot, target):
        i = offset(chip, target)
        return remote(
            chip_send.at[slot, i],
            chip_in.at[slot, i],
            chip_send_sem.at[slot, i],
            chip_recv_sem.at[slot, i],
            (sec, target * 2 + core),
        )

    def ffn_mate(slot):
        return remote(
            x_ffn.at[slot, me], x_ffn.at[slot, me], ffn_mate_send.at[slot], ffn_mate_recv.at[slot], mate
        )

    def ffn_direct(slot, target):
        i = offset(chip, target)
        return remote(
            x_ffn.at[slot, me],
            x_ffn.at[slot, me],
            ffn_send.at[slot, i],
            ffn_recv.at[slot, i],
            (sec, target * 2 + core),
        )

    def ffn_arrival(slot, o):
        j = o * 2 + core
        i = offset(o, chip)
        return remote(x_ffn.at[slot, j], x_ffn.at[slot, j], ffn_send.at[slot, i], ffn_recv.at[slot, i], mate)

    def ffn_relay(slot, o, by):
        j = o * 2 + by
        i = offset(o, chip)
        return remote(
            x_ffn.at[slot, j], x_ffn.at[slot, j], ffn_relay_send.at[slot, i], ffn_relay_recv.at[slot, i], mate
        )

    def project(m):
        slot = m % 2
        squares[...] = jnp.zeros_like(squares)

        @pl.when((sec == 0) & (m != 0))
        def _():
            remote(x_in.at[m], x_in.at[m], seed_send, seed_recv.at[m], mate).wait_recv()

        def direct(i, _):
            o = nth(near, i)

            @pl.when(sec != 0)
            def _():
                x_direct(m, o, mate).wait_recv()
                x_relay(m, o).start()

            j = o * 2 + core
            scaled[:, columns(j)] = with_gain(0, j, x_in[m, j])
            return 0

        lax.fori_loop(0, chips, direct, 0)

        def relayed(i, _):
            o = nth(near, i)

            @pl.when(sec != 0)
            def _():
                x_relayed(m, o).wait_recv()

            j = o * 2 + 1 - core
            scaled[:, columns(j)] = with_gain(0, j, x_in[m, j])
            return 0

        lax.fori_loop(0, chips, relayed, 0)

        @pl.when(sec == 0)
        def _():
            when_loaded(m, 0, 2)

        when_loaded(m, 2, 3)
        scale = row_scale()
        left = scaled[...]
        kv = (jnp.dot(left, v_kv[...], preferred_element_type=F32) * scale).astype(BF16)

        @pl.when(sec == 0)
        def _():
            stacked = jnp.concatenate([kv[:, :key_width], kv[:, key_width:]], axis=0)
            by_head = lax.dot_general(
                pick, stacked, (((1,), (1,)), ((), ())), preferred_element_type=F32
            )
            kv_send[slot] = by_head.astype(BF16).reshape(KV_HEADS, parts_here, 2 * length)
            for step in range(1, peers):
                kv_copy(slot, step).start()
            kv_recv[slot, me] = kv_send[slot, me]

        @pl.when(sec != 0)
        def _():
            key = kv[:, :key_width].astype(F32)
            key_buf[...] = (key * q_cos[...] + pltpu.roll(key, HD // 2, 1) * q_sin[...]).astype(BF16)
            value_buf[...] = kv[:, key_width:]

        query = jnp.dot(left, v_query[...], preferred_element_type=F32) * scale
        for h in range(heads_here):
            head = query[:, h * HD : (h + 1) * HD]
            query_buf[slot, pl.ds(h * length, length), :] = (
                head * q_cos[...] + pltpu.roll(head, HD // 2, 1) * q_sin[...]
            ).astype(BF16)

    def attend(m):
        slot = m % 2

        def mix(key, value, value_side, shift):
            sides = (((1,), (1 - value_side,)), ((), ()))
            scores = lax.dot_general(query_buf[slot], key, sides, preferred_element_type=F32) * HD ** (-0.5)
            token = lax.broadcasted_iota(jnp.int32, scores.shape, 0) % length
            key_at = lax.broadcasted_iota(jnp.int32, scores.shape, 1)
            scores = jnp.where(key_at <= token, scores, -jnp.inf)
            scores = jnp.exp(scores - jnp.max(scores, axis=-1, keepdims=True))
            chances = scores / jnp.sum(scores, axis=-1, keepdims=True)
            if shift:
                chances = pltpu.roll(chances, length, 1)
            mixed_buf[...] = lax.dot_general(
                chances.astype(BF16), value, (((1,), (value_side,)), ((), ())), preferred_element_type=F32
            )

        @pl.when(sec == 0)
        def _():
            for step in range(1, peers):
                kv_copy(slot, step).wait()
            pair = kv_recv[slot].reshape(HD, 2 * length).astype(F32)
            swapped = jnp.concatenate([pair[HD // 2 :], pair[: HD // 2]], axis=0)
            pair = (pair * k_cos[...] + swapped * k_sin[...]).astype(BF16)
            mix(pair, pair, 1, True)

        @pl.when(sec != 0)
        def _():
            mix(key_buf[...], value_buf[...], 0, False)

        mixed = mixed_buf[...]
        for h in range(heads_here):
            on = me * heads_here + h < heads_on[0, m]
            rows = mixed[h * length : (h + 1) * length]
            context[:, h * HD : (h + 1) * HD] = jnp.where(on, rows, 0.0).astype(BF16)
        when_loaded(m, 3, 4)
        scatter(slot, context, v_out, x_in[m, me].astype(F32))

    def scatter(slot, left, weight, base):
        def to_mate(k, _):
            at = columns(nth(far, k) * 2 + 1 - core)
            pair_send[slot, k] = jnp.dot(left[...], weight[:, at], preferred_element_type=F32).astype(BF16)
            pair_copy(slot, k).start()
            return 0

        lax.fori_loop(0, chips, to_mate, 0)

        def to_chip(k, _):
            target = nth(far, k)
            term = jnp.dot(left[...], weight[:, columns(target * 2 + core)], preferred_element_type=F32)
            pair_copy(slot, k).wait_recv()
            i = offset(chip, target)
            chip_send[slot, i] = (term + pair_in[slot, k].astype(F32)).astype(BF16)
            chip_copy(slot, target).start()
            return 0

        lax.fori_loop(0, chips - 1, to_chip, 0)
        term = jnp.dot(left[...], weight[:, columns(me)], preferred_element_type=F32)
        residual[slot] = base + term

    def gathered_sum(slot):
        for k in range(chips):
            pair_copy(slot, k).wait_send()
        pair_copy(slot, chips - 1).wait_recv()
        total = residual[slot] + pair_in[slot, chips - 1].astype(F32)
        for k in range(chips - 1):
            pltpu.make_async_copy(chip_in.at[slot, k], chip_in.at[slot, k], chip_recv_sem.at[slot, k]).wait()
            total = total + chip_in[slot, k].astype(F32)
            pltpu.make_async_copy(chip_send.at[slot, k], chip_send.at[slot, k], chip_send_sem.at[slot, k]).wait()
        return total

    def share(m):
        slot = m % 2
        attended = gathered_sum(slot)
        residual[slot] = attended
        x_ffn[slot, me] = attended.astype(BF16)
        for o in near[1:]:
            ffn_direct(slot, o).start()
        ffn_mate(slot).start()

    def feed_forward(m):
        slot = m % 2
        when_loaded(m, 4, 6)
        squares[...] = jnp.zeros_like(squares)

        def piece(j, first):
            left = with_gain(1, j, x_ffn[slot, j])
            rows = columns(j)
            for weight, acc in ((v_gate, acc_gate), (v_up, acc_up)):
                term = jnp.dot(left, weight[rows, :], preferred_element_type=F32)
                acc[...] = term if first else acc[...] + term

        piece(me, True)
        ffn_mate(slot).wait_recv()
        piece(mate_at, False)

        def from_chip(i, _):
            o = nth(near, i)
            ffn_arrival(slot, o).wait_recv()
            ffn_relay(slot, o, core).start()
            piece(o * 2 + core, False)
            ffn_relay(slot, o, 1 - core).wait_recv()
            piece(o * 2 + 1 - core, False)
            return 0

        lax.fori_loop(1, chips, from_chip, 0)
        scale = row_scale()
        active = BLOCK * ffn_blocks[0, m]

        def activate(i, _):
            at = pl.ds(pl.multiple_of(i * TILE, TILE), TILE)
            gate = acc_gate[:, at] * scale
            up = acc_up[:, at] * scale
            unit = me * units + i * TILE + lax.broadcasted_iota(jnp.int32, gate.shape, 1)
            value = gate / (1.0 + jnp.exp(-gate)) * up
            hidden[:, at] = jnp.where(unit < active, value, 0.0).astype(BF16)
            return 0

        lax.fori_loop(0, units // TILE, activate, 0)
        when_loaded(m, 6, 7)
        scatter(slot, hidden, v_down, residual[slot])
        ffn_mate(slot).wait_send()
        for o in near[1:]:
            ffn_direct(slot, o).wait_send()
            ffn_relay(slot, o, core).wait_send()

    def hand_over(m):
        result[m] = gathered_sum(m % 2).astype(BF16)
        for o in near:
            here = (sec == last) & (m == last) & (o == chip)

            @pl.when(sec < last)
            def _():
                remote(
                    result.at[m], x_in.at[m, me], result_send.at[m, o], x_recv.at[m, chip], (sec + 1, o * 2 + core)
                ).start()

            if o is not chip:

                @pl.when(sec == last)
                def _():
                    remote(
                        result.at[m], final.at[me], result_send.at[m, o], final_recv.at[chip], (m, o * 2 + core)
                    ).start()

        @pl.when((sec == last) & (m != last))
        def _():
            remote(
                result.at[m], final.at[me], result_send.at[m, chip], final_recv.at[chip], (m, me)
            ).start()

        @pl.when((sec == last) & (m == last))
        def _():
            pltpu.make_async_copy(result.at[m], final.at[me], final_recv.at[chip]).start()

    def when_loaded(m, first, stop):
        @pl.when(m == 0)
        def _():
            for copy in weight_copies()[first:stop]:
                copy.wait()

    def micro_step(m, _):
        @pl.when((sec != 0) | (m == 0))
        def _():
            project(m)

        attend(m)

        @pl.when((sec == 0) & (m < last))
        def _():
            project(m + 1)

        share(m)
        feed_forward(m)
        hand_over(m)
        return 0

    lax.fori_loop(0, sections, micro_step, 0)

    def drain(m, _):
        for o in range(chips):

            @pl.when((sec < last) | (m < last) | (o != chip))
            def _():
                remote(result.at[m], final.at[me], result_send.at[m, o], final_recv.at[chip], mate).wait_send()

            @pl.when(sec != 0)
            def _():
                x_relay(m, o).wait_send()

        return 0

    lax.fori_loop(0, sections, drain, 0)

    def final_copy(o, by):
        j = o * 2 + by
        return remote(final.at[j], final.at[j], final_relay_send.at[o], final_relay_recv.at[o], mate)

    def to_output(j):
        return pltpu.make_async_copy(final.at[j], out.at[:, columns(j)], out_sem.at[j])

    for o in near:
        j = o * 2 + core
        remote(final.at[j], final.at[j], result_send.at[0, o], final_recv.at[o], mate).wait_recv()
        final_copy(o, core).start()
        to_output(j).start()
    for o in near:
        final_copy(o, 1 - core).wait_recv()
        to_output(o * 2 + 1 - core).start()
    for o in near:
        final_copy(o, core).wait_send()
    for j in range(peers):
        to_output(j).wait()


def resident(hidden_in, attn_gain, w_query, w_key, w_value, w_out, ffn_gain, w_gate, w_up, w_down, ffn_blocks, heads_on):
    sections, peers = lax.axis_size("section"), lax.axis_size("mp")
    length, width = hidden_in.shape[2:]
    block, chips = width // peers, peers // 2
    units, key_width = w_gate.shape[2], w_key.shape[2]
    query_width = w_query.shape[2]
    parts_here = key_width // KV_HEADS
    vmem = pl.BlockSpec(memory_space=pltpu.VMEM)
    hbm = pl.BlockSpec(memory_space=pl.ANY)
    dma = pltpu.SemaphoreType.DMA
    half = pltpu.VMEM
    result = pl.pallas_call(
        lambda *refs: layer_kernel(sections, peers, *refs),
        out_shape=jax.ShapeDtypeStruct((length, width), BF16),
        in_specs=[hbm] * 3 + [vmem] * 6 + [hbm] * 7,
        out_specs=hbm,
        scratch_shapes=[
            half((width, query_width), BF16),
            half((width, 2 * key_width), BF16),
            half((query_width, width), BF16),
            half((width, units), BF16),
            half((width, units), BF16),
            half((units, width), BF16),
            pltpu.SMEM((1, sections), jnp.int32),
            pltpu.SMEM((1, sections), jnp.int32),
            half((2, peers, 8, block), F32),
            half((sections, peers, length, block), BF16),
            half((2, peers, length, block), BF16),
            half((peers, length, block), BF16),
            half((length, width), BF16),
            half((length, HD), F32),
            half((2, length, block), F32),
            half((2, query_width // HD * length, HD), BF16),
            half((length, HD), BF16),
            half((length, HD), BF16),
            half((query_width // HD * length, HD), F32),
            half((2, peers, parts_here, 2 * length), BF16),
            half((2, peers, parts_here, 2 * length), BF16),
            half((length, query_width), BF16),
            half((length, units), F32),
            half((length, units), F32),
            half((length, units), BF16),
            half((2, chips, length, block), BF16),
            half((2, chips, length, block), BF16),
            half((2, chips - 1, length, block), BF16),
            half((2, chips - 1, length, block), BF16),
            half((sections, length, block), BF16),
            dma((7,)),
            dma((2, peers - 1)),
            dma((2, peers - 1)),
            dma((2,)),
            dma((peers,)),
            dma,
            dma((sections,)),
            dma((sections, chips)),
            dma((sections, chips)),
            dma((sections, chips)),
            dma((2, peers - 1)),
            dma((2, peers - 1)),
            dma((2, chips)),
            dma((2, chips)),
            dma((2, chips - 1)),
            dma((2, chips - 1)),
            dma((2,)),
            dma((2,)),
            dma((2, chips - 1)),
            dma((2, chips - 1)),
            dma((2, chips - 1)),
            dma((2, chips - 1)),
            dma((sections, chips)),
            dma((chips,)),
            dma((chips,)),
            dma((chips,)),
            dma((peers,)),
        ],
        compiler_params=pltpu.CompilerParams(
            collective_id=0, has_side_effects=True, vmem_limit_bytes=67043328
        ),
    )(
        heads_on.T,
        ffn_blocks.T,
        hidden_in.reshape(length, width),
        attn_gain,
        ffn_gain,
        *tables(length),
        w_query[0],
        w_key[0],
        w_value[0],
        w_out[0],
        w_gate[0],
        w_up[0],
        w_down[0],
    )
    return result.reshape(hidden_in.shape)


def one_device(*args):
    hidden_in, w_query, w_key, w_gate = args[0], args[2], args[3], args[7]
    sections, peers = lax.axis_size("section"), lax.axis_size("mp")
    fits = (
        hidden_in.shape[0] == 1
        and args[10].shape[0] == sections
        and peers == KV_HEADS
        and sections == 4
        and args[5].shape[1] == w_query.shape[2]
        and 2 * hidden_in.shape[2] == HD
        and w_query.shape[2] * KV_HEADS == HEADS * HD
        and w_key.shape[2] == HD
        and w_gate.shape[2] % TILE == 0
        and hidden_in.shape[3] % (peers * HD) == 0
        and hidden_in.shape[3] == HEADS * HD
    )
    return (resident if fits else per_device)(*args)


def solution(mesh):
    return jax.shard_map(
        one_device,
        mesh=mesh,
        in_specs=(
            P(None, "section", None, None),
            P("section", None),
            P("section", None, "mp"),
            P("section", None, "mp"),
            P("section", None, "mp"),
            P("section", "mp", None),
            P("section", None),
            P("section", None, "mp"),
            P("section", None, "mp"),
            P("section", "mp", None),
            P(None, "section"),
            P(None, "section"),
        ),
        out_specs=P(None, "section", None, None),
        check_vma=False,
    )
```

```python
import jax
import jax.numpy as jnp
import numpy as np
from jax import lax
from jax.experimental import pallas as pl
from jax.experimental.pallas import tpu as pltpu
from jax.sharding import PartitionSpec as P

HEADS = 32
KV_HEADS = 8
HD = 128
BLOCK = 128


ROPE_BASE = 500000.0
EPSILON = 1e-05


def passed_along(array, axis, by):
    peers = lax.axis_size(axis)
    return lax.ppermute(array, axis, [(i, (i + by) % peers) for i in range(peers)])


def rms_scale(values, gain_row):
    mean_sq = jnp.mean(values * values, axis=-1, keepdims=True)
    return values * lax.rsqrt(mean_sq + EPSILON) * gain_row.astype(jnp.float32)


def rotate(values):
    length = values.shape[0]
    half_dim = values.shape[-1] // 2
    frequency = ROPE_BASE ** (-(jnp.arange(half_dim, dtype=jnp.float32) / half_dim))
    angles = jnp.arange(length, dtype=jnp.float32)[:, None] * frequency[None, :]
    cosine_table = jnp.cos(angles)[:, None, :]
    sine_table = jnp.sin(angles)[:, None, :]
    front_half = values[..., :half_dim].astype(jnp.float32)
    back_half = values[..., half_dim:].astype(jnp.float32)
    return jnp.concatenate(
        [
            front_half * cosine_table - back_half * sine_table,
            front_half * sine_table + back_half * cosine_table,
        ],
        axis=-1,
    )


def attend_local(projected, query_width, key_width, active, first_head):
    length = projected.shape[0]
    heads_here = query_width // HD
    group_size = HEADS // KV_HEADS
    queries = rotate(projected[:, :query_width].reshape(length, heads_here, HD)).astype(
        jnp.bfloat16
    )
    key_local = projected[:, query_width : query_width + key_width].astype(jnp.bfloat16)
    value_local = projected[:, query_width + key_width :].astype(jnp.bfloat16)
    key_whole, value_whole = (
        lax.all_gather(key_local, "mp", axis=1, tiled=True),
        lax.all_gather(value_local, "mp", axis=1, tiled=True),
    )
    key_heads = key_whole.reshape(length, HD, KV_HEADS).transpose(0, 2, 1)
    value_heads = value_whole.reshape(length, HD, KV_HEADS).transpose(0, 2, 1)
    kv_here = max(1, heads_here // group_size)
    repeat_count = heads_here // kv_here
    first_kv = first_head // group_size
    key_pick = lax.dynamic_slice_in_dim(key_heads, first_kv, kv_here, 1)
    value_pick = lax.dynamic_slice_in_dim(value_heads, first_kv, kv_here, 1)
    keys_rot = jnp.repeat(rotate(key_pick).astype(jnp.bfloat16), repeat_count, axis=1)
    values = jnp.repeat(value_pick, repeat_count, axis=1)
    scores = jnp.einsum(
        "qhd,khd->hqk", queries, keys_rot, preferred_element_type=jnp.float32
    ) * HD ** (-0.5)
    causal = jnp.arange(length)[:, None] >= jnp.arange(length)[None, :]
    scores = jnp.where(causal[None], scores, -jnp.inf)
    probabilities = jax.nn.softmax(scores, axis=-1).astype(jnp.bfloat16)
    context = jnp.einsum("hqk,khd->qhd", probabilities, values, preferred_element_type=jnp.float32)
    head_ids = first_head + jnp.arange(heads_here)
    context = jnp.where((head_ids < active)[None, :, None], context, 0.0).astype(jnp.bfloat16)
    return context.reshape(length, query_width)


def per_device(
    hidden_in,
    attn_gain,
    w_query,
    w_key,
    w_value,
    w_out,
    ffn_gain,
    w_gate,
    w_up,
    w_down,
    ffn_blocks,
    heads_on,
):
    section_count = lax.axis_size("section")
    section_index = lax.axis_index("section")
    model_count = lax.axis_size("mp")
    model_index = lax.axis_index("mp")
    micro_total = ffn_blocks.shape[0]
    per_section = hidden_in.shape[0]
    length = hidden_in.shape[2]
    model_width = hidden_in.shape[3]
    local_rows = length // model_count
    units_here = w_gate.shape[2]
    query_width = w_query.shape[2]
    key_width = w_key.shape[2]
    first_head = model_index * (query_width // HD)
    first_unit = model_index * units_here
    joined_qkv = [jnp.concatenate([w_query[0], w_key[0], w_value[0]], axis=1)]
    joined_pair = [jnp.concatenate([w_gate[0], w_up[0]], axis=1)]

    def gated(pre_act, block_count):
        gate_part = pre_act[:, :units_here]
        up_part = pre_act[:, units_here:]
        unit_ids = first_unit + jnp.arange(units_here)
        return jnp.where(
            (unit_ids < BLOCK * block_count)[None, :], jax.nn.silu(gate_part) * up_part, 0.0
        ).astype(jnp.bfloat16)

    def layer_rows(carried, layer_pos, active, block_count):
        residual = carried.astype(jnp.float32)
        normed = rms_scale(residual, attn_gain[layer_pos]).astype(jnp.bfloat16)
        projected = jnp.dot(
            lax.all_gather(normed, "mp", axis=0, tiled=True),
            joined_qkv[layer_pos],
            preferred_element_type=jnp.float32,
        )
        context = attend_local(projected, query_width, key_width, active, first_head)
        attended = residual + lax.psum_scatter(
            jnp.dot(context, w_out[layer_pos], preferred_element_type=jnp.float32).astype(
                jnp.bfloat16
            ),
            "mp",
            scatter_dimension=0,
            tiled=True,
        ).astype(jnp.float32)
        normed_ffn = rms_scale(attended, ffn_gain[layer_pos]).astype(jnp.bfloat16)
        hidden = gated(
            jnp.dot(
                lax.all_gather(normed_ffn, "mp", axis=0, tiled=True),
                joined_pair[layer_pos],
                preferred_element_type=jnp.float32,
            ),
            block_count,
        )
        return (
            attended
            + lax.psum_scatter(
                jnp.dot(hidden, w_down[layer_pos], preferred_element_type=jnp.float32).astype(
                    jnp.bfloat16
                ),
                "mp",
                scatter_dimension=0,
                tiled=True,
            ).astype(jnp.float32)
        ).astype(jnp.bfloat16)

    def section_work(carried, moment, layer_fn):
        micro_index = jnp.clip(moment - section_index, 0, micro_total - 1)
        carried = layer_fn(carried, 0, heads_on[micro_index, 0], ffn_blocks[micro_index, 0])
        return carried

    def tick_step(moment, loop_carry):
        carried, slot_buffer = loop_carry
        cycle_index = moment // section_count
        incoming = lax.dynamic_index_in_dim(
            slot_buffer, jnp.minimum(cycle_index, per_section - 1), 0, keepdims=False
        )
        incoming = jnp.where(moment < micro_total, incoming, jnp.zeros_like(incoming))
        at_head = section_index == 0
        written = lax.dynamic_update_index_in_dim(
            slot_buffer, carried, jnp.maximum(cycle_index - 1, 0), 0
        )
        slot_buffer = jnp.where(at_head & (moment >= section_count), written, slot_buffer)
        carried = jnp.where(at_head, incoming, carried)
        carried = section_work(carried, moment, layer_rows)
        carried = passed_along(carried, "section", 1)
        slot_buffer = passed_along(slot_buffer, "section", -1)
        return (carried, slot_buffer)

    slot_start = hidden_in.reshape(per_section, length, model_width)
    slot_start = lax.dynamic_slice_in_dim(slot_start, model_index * local_rows, local_rows, 1)
    initial = jnp.zeros((local_rows, model_width), jnp.bfloat16)
    finished = lax.fori_loop(0, micro_total + section_count, tick_step, (initial, slot_start))
    result = finished[1]
    result = lax.all_gather(result, "mp", axis=1, tiled=True)
    return result.reshape(hidden_in.shape)


MESH = pl.DeviceIdType.MESH
BF16 = jnp.bfloat16
F32 = jnp.float32
TILE = 256


def tables(length):
    half = HD // 2
    frequency = np.float32(ROPE_BASE) ** (-(np.arange(half, dtype=np.float32) / np.float32(half)))
    angles = np.arange(length, dtype=np.float32)[:, None] * frequency[None, :].astype(np.float32)
    cosine, sine = np.cos(angles), np.sin(angles)
    q_cos = np.concatenate([cosine, cosine], axis=1)
    q_sin = np.concatenate([-sine, sine], axis=1)
    k_cos = np.concatenate([q_cos.T, np.ones((HD, length))], axis=1)
    k_sin = np.concatenate([q_sin.T, np.zeros((HD, length))], axis=1)
    return [jnp.asarray(t, F32) for t in (q_cos, q_sin, k_cos, k_sin)]


def remote(src, dst, send_sem, recv_sem, where):
    return pltpu.make_async_remote_copy(
        src_ref=src,
        dst_ref=dst,
        send_sem=send_sem,
        recv_sem=recv_sem,
        device_id=where,
        device_id_type=MESH,
    )


def layer_kernel(
    sections,
    peers,
    heads_hbm,
    blocks_hbm,
    hidden_in,
    attn_gain,
    ffn_gain,
    q_cos,
    q_sin,
    k_cos,
    k_sin,
    w_query,
    w_key,
    w_value,
    w_out,
    w_gate,
    w_up,
    w_down,
    out,
    v_query,
    v_kv,
    v_out,
    v_gate,
    v_up,
    v_down,
    heads_on,
    ffn_blocks,
    gains,
    x_in,
    x_ffn,
    final,
    scaled,
    squares,
    residual,
    query_buf,
    key_buf,
    value_buf,
    mixed_buf,
    kv_send,
    kv_recv,
    context,
    acc_gate,
    acc_up,
    hidden,
    pair_send,
    pair_in,
    chip_send,
    chip_in,
    result,
    weight_sem,
    head_send_sem,
    head_recv_sem,
    small_sem,
    stage_sem,
    seed_send,
    seed_recv,
    x_recv,
    x_relay_send,
    x_relay_recv,
    kv_send_sem,
    kv_recv_sem,
    pair_send_sem,
    pair_recv_sem,
    chip_send_sem,
    chip_recv_sem,
    ffn_mate_send,
    ffn_mate_recv,
    ffn_send,
    ffn_recv,
    ffn_relay_send,
    ffn_relay_recv,
    result_send,
    final_recv,
    final_relay_send,
    final_relay_recv,
    out_sem,
):
    sec = lax.axis_index("section")
    me = lax.axis_index("mp")
    chips = peers // 2
    chip, core = me // 2, me % 2
    mate_at = chip * 2 + 1 - core
    mate = (sec, mate_at)
    last = sections - 1
    length, block = x_in.shape[2:]
    width = peers * block
    heads_here = v_query.shape[1] // HD
    key_width = w_key.shape[1]
    units = v_gate.shape[1]
    high = chip // 2
    near = (chip, chip + 1 - 2 * (chip % 2), 2 - high, 3 * (1 - high))
    far = near[::-1]

    def nth(order, i):
        value = order[0]
        for k in range(1, len(order)):
            value = jnp.where(i == k, order[k], value)
        return value

    def offset(source, target):
        return (source - target + chips) % chips - 1

    def weight_copies():
        pairs = (
            (w_key, v_kv.at[:, pl.ds(0, key_width)]),
            (w_value, v_kv.at[:, pl.ds(key_width, key_width)]),
            (w_query, v_query),
            (w_out, v_out),
            (w_gate, v_gate),
            (w_up, v_up),
            (w_down, v_down),
        )
        return [
            pltpu.make_async_copy(a, b, weight_sem.at[i]) for i, (a, b) in enumerate(pairs)
        ]

    def columns(j):
        return pl.ds(pl.multiple_of(j * block, block), block)

    small = [
        pltpu.make_async_copy(heads_hbm, heads_on, small_sem.at[0]),
        pltpu.make_async_copy(blocks_hbm, ffn_blocks, small_sem.at[1]),
    ]
    for copy in small:
        copy.start()

    def staged(target):
        return [
            pltpu.make_async_copy(hidden_in.at[:, pl.ds(j * block, block)], target.at[j], stage_sem.at[j])
            for j in range(peers)
        ]

    @pl.when(sec == 0)
    def _():
        for copy in staged(x_in.at[0]):
            copy.start()

    @pl.when(sec != 0)
    def _():
        for copy in staged(final):
            copy.start()

    for copy in weight_copies()[:2]:
        copy.start()

    @pl.when(sec == 0)
    def _():
        for copy in weight_copies()[2:]:
            copy.start()

    barrier = pltpu.get_barrier_semaphore()
    for step in range(1, peers):
        pl.semaphore_signal(barrier, inc=1, device_id=(sec, (me + step) % peers), device_id_type=MESH)
    for step in range(1, sections):
        for away in range(chips):
            pl.semaphore_signal(
                barrier,
                inc=1,
                device_id=((sec + step) % sections, (chip + away) % chips * 2 + core),
                device_id_type=MESH,
            )
    pl.semaphore_wait(barrier, peers - 1 + (sections - 1) * chips)

    seed = remote(final, x_in.at[sec], seed_send, seed_recv.at[sec], (0, me))

    @pl.when(sec == 0)
    def _():
        for copy in staged(x_in.at[0]):
            copy.wait()

    @pl.when(sec != 0)
    def _():
        for copy in staged(final):
            copy.wait()
        seed.start()

    for row, gain in enumerate((attn_gain, ffn_gain)):
        for j in range(peers):
            gains[row, j] = jnp.broadcast_to(
                gain[:, j * block : (j + 1) * block].astype(F32), gains.shape[2:]
            )
    for copy in small:
        copy.wait()

    parts_here = key_width // KV_HEADS
    tile_row = lax.broadcasted_iota(jnp.int32, (key_width, key_width), 0)
    tile_col = lax.broadcasted_iota(jnp.int32, (key_width, key_width), 1)
    by_heads = tile_col == tile_row % parts_here * KV_HEADS + tile_row // parts_here
    pick = jnp.where(by_heads, 1.0, 0.0).astype(BF16)
    same = jnp.where(tile_col == tile_row, 1.0, 0.0).astype(BF16)

    def head_rows(which, by, received):
        at = received * 2 * key_width + which * key_width + by * parts_here
        return v_down.at[pl.ds(pl.multiple_of(at, parts_here), parts_here), :]

    def head_copy(which, k, b):
        to = far[k] * 2 + (1 - core if b else core)
        i = offset(chip, far[k]) * 2 + b if k < chips - 1 else peers - 2
        return remote(
            head_rows(which, to, 0),
            head_rows(which, me, 1),
            head_send_sem.at[which, i],
            head_recv_sem.at[which, i],
            (sec, to),
        )

    def head_arrival(which, k, b):
        by = far[k] * 2 + (1 - core if b else core)
        i = offset(far[k], chip) * 2 + b if k < chips - 1 else peers - 2
        there = head_rows(which, by, 1)
        return remote(there, there, head_send_sem.at[which, i], head_recv_sem.at[which, i], mate)

    head_order = [(k, b) for k in range(chips - 1) for b in range(2)] + [(chips - 1, 1)]

    def stripe(i):
        return pl.ds(pl.multiple_of(i * block, block), block)

    @pl.when(sec != 0)
    def _():
        seed.wait_send()
        for copy in weight_copies()[:2]:
            copy.wait()

        for which in range(2):
            rows = pl.ds(which * key_width, key_width)

            def to_heads(i, _):
                turned = lax.dot_general(
                    pick, v_kv[stripe(i), rows], (((1,), (1,)), ((), ())), preferred_element_type=F32
                )
                v_down[rows, stripe(i)] = turned.astype(BF16)
                return 0

            lax.fori_loop(0, peers, to_heads, 0)
            for k, b in head_order:
                head_copy(which, k, b).start()
            own = pl.multiple_of(which * key_width + me * parts_here, parts_here)
            v_down[pl.ds(2 * key_width + own, parts_here), :] = v_down[pl.ds(own, parts_here), :]
        for copy in weight_copies()[2:-1]:
            copy.start()
        for which in range(2):
            for k, b in head_order:
                head_copy(which, k, b).wait_send()
                head_arrival(which, k, b).wait_recv()
            rows = pl.ds(which * key_width, key_width)

            def from_heads(i, _):
                turned = lax.dot_general(
                    v_down[pl.ds((2 + which) * key_width, key_width), stripe(i)],
                    same,
                    (((0,), (0,)), ((), ())),
                    preferred_element_type=F32,
                )
                v_kv[stripe(i), rows] = turned.astype(BF16)
                return 0

            lax.fori_loop(0, peers, from_heads, 0)
        weight_copies()[-1].start()

    def row_scale():
        total = jnp.sum(squares[...], axis=-1, keepdims=True)
        return lax.rsqrt(total * (1.0 / width) + EPSILON)

    def with_gain(row, j, values):
        x = values.astype(F32)
        part = x * x
        total = part[:, :HD]
        for k in range(1, block // HD):
            total = total + part[:, k * HD : (k + 1) * HD]
        squares[...] = squares[...] + total
        return (x * gains[row, j, 0:1, :]).astype(BF16)

    def x_direct(m, o, where):
        j = o * 2 + core
        return remote(x_in.at[m, j], x_in.at[m, j], result_send.at[m, o], x_recv.at[m, o], where)

    def x_relay(m, o):
        j = o * 2 + core
        return remote(x_in.at[m, j], x_in.at[m, j], x_relay_send.at[m, o], x_relay_recv.at[m, o], mate)

    def x_relayed(m, o):
        j = o * 2 + 1 - core
        return remote(x_in.at[m, j], x_in.at[m, j], x_relay_send.at[m, o], x_relay_recv.at[m, o], mate)

    def kv_copy(slot, step):
        to = (me + step) % peers
        return remote(
            kv_send.at[slot, to],
            kv_recv.at[slot, me],
            kv_send_sem.at[slot, step - 1],
            kv_recv_sem.at[slot, step - 1],
            (sec, to),
        )

    def pair_copy(m, k):
        return remote(
            pair_send.at[m % 2, k], pair_in.at[m, k], pair_send_sem.at[m, k], pair_recv_sem.at[m, k], mate
        )

    def chip_copy(m, target):
        i = offset(chip, target)
        return remote(
            chip_send.at[m % 2, i],
            chip_in.at[m, i],
            chip_send_sem.at[m, i],
            chip_recv_sem.at[m, i],
            (sec, target * 2 + core),
        )

    def ffn_mate(slot):
        return remote(
            x_ffn.at[slot, me], x_ffn.at[slot, me], ffn_mate_send.at[slot], ffn_mate_recv.at[slot], mate
        )

    def ffn_direct(slot, target):
        i = offset(chip, target)
        return remote(
            x_ffn.at[slot, me],
            x_ffn.at[slot, me],
            ffn_send.at[slot, i],
            ffn_recv.at[slot, i],
            (sec, target * 2 + core),
        )

    def ffn_arrival(slot, o):
        j = o * 2 + core
        i = offset(o, chip)
        return remote(x_ffn.at[slot, j], x_ffn.at[slot, j], ffn_send.at[slot, i], ffn_recv.at[slot, i], mate)

    def ffn_relay(slot, o, by):
        j = o * 2 + by
        i = offset(o, chip)
        return remote(
            x_ffn.at[slot, j], x_ffn.at[slot, j], ffn_relay_send.at[slot, i], ffn_relay_recv.at[slot, i], mate
        )

    def project(m):
        slot = m % 2
        squares[...] = jnp.zeros_like(squares)

        @pl.when((sec == 0) & (m != 0))
        def _():
            remote(x_in.at[m], x_in.at[m], seed_send, seed_recv.at[m], mate).wait_recv()

        def direct(i, _):
            o = nth(near, i)

            @pl.when(sec != 0)
            def _():
                x_direct(m, o, mate).wait_recv()
                x_relay(m, o).start()

            j = o * 2 + core
            scaled[:, columns(j)] = with_gain(0, j, x_in[m, j])
            return 0

        lax.fori_loop(0, chips, direct, 0)

        def relayed(i, _):
            o = nth(near, i)

            @pl.when(sec != 0)
            def _():
                x_relayed(m, o).wait_recv()

            j = o * 2 + 1 - core
            scaled[:, columns(j)] = with_gain(0, j, x_in[m, j])
            return 0

        lax.fori_loop(0, chips, relayed, 0)

        @pl.when(sec == 0)
        def _():
            when_loaded(m, 0, 2)

        when_loaded(m, 2, 3)
        scale = row_scale()
        left = scaled[...]
        kv = (jnp.dot(left, v_kv[...], preferred_element_type=F32) * scale).astype(BF16)

        @pl.when(sec == 0)
        def _():
            stacked = jnp.concatenate([kv[:, :key_width], kv[:, key_width:]], axis=0)
            by_head = lax.dot_general(
                pick, stacked, (((1,), (1,)), ((), ())), preferred_element_type=F32
            )
            kv_send[slot] = by_head.astype(BF16).reshape(KV_HEADS, parts_here, 2 * length)
            for step in range(1, peers):
                kv_copy(slot, step).start()
            kv_recv[slot, me] = kv_send[slot, me]

        @pl.when(sec != 0)
        def _():
            key = kv[:, :key_width].astype(F32)
            key_buf[...] = (key * q_cos[...] + pltpu.roll(key, HD // 2, 1) * q_sin[...]).astype(BF16)
            value_buf[...] = kv[:, key_width:]

        query = jnp.dot(left, v_query[...], preferred_element_type=F32) * scale
        for h in range(heads_here):
            head = query[:, h * HD : (h + 1) * HD]
            query_buf[slot, pl.ds(h * length, length), :] = (
                head * q_cos[...] + pltpu.roll(head, HD // 2, 1) * q_sin[...]
            ).astype(BF16)

    def attend(m):
        slot = m % 2

        def mix(key, value, value_side, shift):
            sides = (((1,), (1 - value_side,)), ((), ()))
            scores = lax.dot_general(query_buf[slot], key, sides, preferred_element_type=F32) * HD ** (-0.5)
            token = lax.broadcasted_iota(jnp.int32, scores.shape, 0) % length
            key_at = lax.broadcasted_iota(jnp.int32, scores.shape, 1)
            scores = jnp.where(key_at <= token, scores, -jnp.inf)
            scores = jnp.exp(scores - jnp.max(scores, axis=-1, keepdims=True))
            chances = scores / jnp.sum(scores, axis=-1, keepdims=True)
            if shift:
                chances = pltpu.roll(chances, length, 1)
            mixed_buf[...] = lax.dot_general(
                chances.astype(BF16), value, (((1,), (value_side,)), ((), ())), preferred_element_type=F32
            )

        @pl.when(sec == 0)
        def _():
            for step in range(1, peers):
                kv_copy(slot, step).wait()
            pair = kv_recv[slot].reshape(HD, 2 * length).astype(F32)
            swapped = jnp.concatenate([pair[HD // 2 :], pair[: HD // 2]], axis=0)
            pair = (pair * k_cos[...] + swapped * k_sin[...]).astype(BF16)
            mix(pair, pair, 1, True)

        @pl.when(sec != 0)
        def _():
            mix(key_buf[...], value_buf[...], 0, False)

        mixed = mixed_buf[...]
        for h in range(heads_here):
            on = me * heads_here + h < heads_on[0, m]
            rows = mixed[h * length : (h + 1) * length]
            context[:, h * HD : (h + 1) * HD] = jnp.where(on, rows, 0.0).astype(BF16)
        when_loaded(m, 3, 4)
        scatter(m, context, v_out, x_in[m, me].astype(F32))

    def scatter(m, left, weight, base):
        def to_mate(k, _):
            at = columns(nth(far, k) * 2 + 1 - core)
            pair_send[m % 2, k] = jnp.dot(left[...], weight[:, at], preferred_element_type=F32).astype(BF16)
            pair_copy(m, k).start()
            return 0

        lax.fori_loop(0, chips, to_mate, 0)

        def to_chip(k, _):
            target = nth(far, k)
            term = jnp.dot(left[...], weight[:, columns(target * 2 + core)], preferred_element_type=F32)
            pair_copy(m, k).wait_recv()
            i = offset(chip, target)
            chip_send[m % 2, i] = (term + pair_in[m, k].astype(F32)).astype(BF16)
            chip_copy(m, target).start()
            return 0

        lax.fori_loop(0, chips - 1, to_chip, 0)
        term = jnp.dot(left[...], weight[:, columns(me)], preferred_element_type=F32)
        residual[m % 2] = base + term

    def gathered_sum(m):
        for k in range(chips):
            pair_copy(m, k).wait_send()
        pair_copy(m, chips - 1).wait_recv()
        total = residual[m % 2] + pair_in[m, chips - 1].astype(F32)
        for k in range(chips - 1):
            pltpu.make_async_copy(chip_in.at[m, k], chip_in.at[m, k], chip_recv_sem.at[m, k]).wait()
            total = total + chip_in[m, k].astype(F32)
            pltpu.make_async_copy(chip_send.at[m % 2, k], chip_send.at[m % 2, k], chip_send_sem.at[m, k]).wait()
        return total

    def share(m):
        slot = m % 2
        attended = gathered_sum(m)
        residual[slot] = attended
        x_ffn[slot, me] = attended.astype(BF16)
        for o in near[1:]:
            ffn_direct(slot, o).start()
        ffn_mate(slot).start()

    def feed_forward(m):
        slot = m % 2
        when_loaded(m, 4, 6)
        squares[...] = jnp.zeros_like(squares)

        def piece(j, first):
            left = with_gain(1, j, x_ffn[slot, j])
            rows = columns(j)
            for weight, acc in ((v_gate, acc_gate), (v_up, acc_up)):
                term = jnp.dot(left, weight[rows, :], preferred_element_type=F32)
                acc[...] = term if first else acc[...] + term

        piece(me, True)
        ffn_mate(slot).wait_recv()
        piece(mate_at, False)

        def from_chip(i, _):
            o = nth(near, i)
            ffn_arrival(slot, o).wait_recv()
            ffn_relay(slot, o, core).start()
            piece(o * 2 + core, False)
            ffn_relay(slot, o, 1 - core).wait_recv()
            piece(o * 2 + 1 - core, False)
            return 0

        lax.fori_loop(1, 3, from_chip, 0)

        @pl.when(m % 2 == 0)
        def _():
            share(m + 1)

        lax.fori_loop(3, chips, from_chip, 0)
        scale = row_scale()
        active = BLOCK * ffn_blocks[0, m]

        def activate(i, _):
            at = pl.ds(pl.multiple_of(i * TILE, TILE), TILE)
            gate = acc_gate[:, at] * scale
            up = acc_up[:, at] * scale
            unit = me * units + i * TILE + lax.broadcasted_iota(jnp.int32, gate.shape, 1)
            value = gate / (1.0 + jnp.exp(-gate)) * up
            hidden[:, at] = jnp.where(unit < active, value, 0.0).astype(BF16)
            return 0

        lax.fori_loop(0, units // TILE, activate, 0)
        when_loaded(m, 6, 7)

        @pl.when(m % 2 == 1)
        def _():
            hand_over(m - 1)

        scatter(m, hidden, v_down, residual[slot])
        ffn_mate(slot).wait_send()
        for o in near[1:]:
            ffn_direct(slot, o).wait_send()
            ffn_relay(slot, o, core).wait_send()

    def hand_over(m):
        result[m] = gathered_sum(m).astype(BF16)
        for o in near:
            here = (sec == last) & (m == last) & (o == chip)

            @pl.when(sec < last)
            def _():
                remote(
                    result.at[m], x_in.at[m, me], result_send.at[m, o], x_recv.at[m, chip], (sec + 1, o * 2 + core)
                ).start()

            if o is not chip:

                @pl.when(sec == last)
                def _():
                    remote(
                        result.at[m], final.at[me], result_send.at[m, o], final_recv.at[chip], (m, o * 2 + core)
                    ).start()

        @pl.when((sec == last) & (m != last))
        def _():
            remote(
                result.at[m], final.at[me], result_send.at[m, chip], final_recv.at[chip], (m, me)
            ).start()

        @pl.when((sec == last) & (m == last))
        def _():
            pltpu.make_async_copy(result.at[m], final.at[me], final_recv.at[chip]).start()

    def when_loaded(m, first, stop):
        @pl.when(m == 0)
        def _():
            for copy in weight_copies()[first:stop]:
                copy.wait()

    def both(g, _):
        def first_half(i, _):
            @pl.when(i < 2)
            def _():
                project(2 * g + i)

            now = jnp.where(sec == 0, i - 1, i)

            @pl.when((now >= 0) & (now < 2))
            def _():
                attend(2 * g + now)

            @pl.when(now == 0)
            def _():
                share(2 * g)

            return 0

        def second_half(i, _):
            feed_forward(2 * g + i)
            return 0

        lax.fori_loop(0, 3, first_half, 0)
        lax.fori_loop(0, 2, second_half, 0)
        hand_over(2 * g + 1)
        return 0

    lax.fori_loop(0, sections // 2, both, 0)

    def drain(m, _):
        for o in range(chips):

            @pl.when((sec < last) | (m < last) | (o != chip))
            def _():
                remote(result.at[m], final.at[me], result_send.at[m, o], final_recv.at[chip], mate).wait_send()

            @pl.when(sec != 0)
            def _():
                x_relay(m, o).wait_send()

        return 0

    lax.fori_loop(0, sections, drain, 0)

    def final_copy(o, by):
        j = o * 2 + by
        return remote(final.at[j], final.at[j], final_relay_send.at[o], final_relay_recv.at[o], mate)

    def to_output(j):
        return pltpu.make_async_copy(final.at[j], out.at[:, columns(j)], out_sem.at[j])

    for o in near:
        j = o * 2 + core
        remote(final.at[j], final.at[j], result_send.at[0, o], final_recv.at[o], mate).wait_recv()
        final_copy(o, core).start()
        to_output(j).start()
    for o in near:
        final_copy(o, 1 - core).wait_recv()
        to_output(o * 2 + 1 - core).start()
    for o in near:
        final_copy(o, core).wait_send()
    for j in range(peers):
        to_output(j).wait()


def resident(hidden_in, attn_gain, w_query, w_key, w_value, w_out, ffn_gain, w_gate, w_up, w_down, ffn_blocks, heads_on):
    sections, peers = lax.axis_size("section"), lax.axis_size("mp")
    length, width = hidden_in.shape[2:]
    block, chips = width // peers, peers // 2
    units, key_width = w_gate.shape[2], w_key.shape[2]
    query_width = w_query.shape[2]
    parts_here = key_width // KV_HEADS
    vmem = pl.BlockSpec(memory_space=pltpu.VMEM)
    hbm = pl.BlockSpec(memory_space=pl.ANY)
    dma = pltpu.SemaphoreType.DMA
    half = pltpu.VMEM
    result = pl.pallas_call(
        lambda *refs: layer_kernel(sections, peers, *refs),
        out_shape=jax.ShapeDtypeStruct((length, width), BF16),
        in_specs=[hbm] * 3 + [vmem] * 6 + [hbm] * 7,
        out_specs=hbm,
        scratch_shapes=[
            half((width, query_width), BF16),
            half((width, 2 * key_width), BF16),
            half((query_width, width), BF16),
            half((width, units), BF16),
            half((width, units), BF16),
            half((units, width), BF16),
            pltpu.SMEM((1, sections), jnp.int32),
            pltpu.SMEM((1, sections), jnp.int32),
            half((2, peers, 8, block), F32),
            half((sections, peers, length, block), BF16),
            half((2, peers, length, block), BF16),
            half((peers, length, block), BF16),
            half((length, width), BF16),
            half((length, HD), F32),
            half((2, length, block), F32),
            half((2, query_width // HD * length, HD), BF16),
            half((length, HD), BF16),
            half((length, HD), BF16),
            half((query_width // HD * length, HD), F32),
            half((2, peers, parts_here, 2 * length), BF16),
            half((2, peers, parts_here, 2 * length), BF16),
            half((length, query_width), BF16),
            half((length, units), F32),
            half((length, units), F32),
            half((length, units), BF16),
            half((2, chips, length, block), BF16),
            half((sections, chips, length, block), BF16),
            half((2, chips - 1, length, block), BF16),
            half((sections, chips - 1, length, block), BF16),
            half((sections, length, block), BF16),
            dma((7,)),
            dma((2, peers - 1)),
            dma((2, peers - 1)),
            dma((2,)),
            dma((peers,)),
            dma,
            dma((sections,)),
            dma((sections, chips)),
            dma((sections, chips)),
            dma((sections, chips)),
            dma((2, peers - 1)),
            dma((2, peers - 1)),
            dma((sections, chips)),
            dma((sections, chips)),
            dma((sections, chips - 1)),
            dma((sections, chips - 1)),
            dma((2,)),
            dma((2,)),
            dma((2, chips - 1)),
            dma((2, chips - 1)),
            dma((2, chips - 1)),
            dma((2, chips - 1)),
            dma((sections, chips)),
            dma((chips,)),
            dma((chips,)),
            dma((chips,)),
            dma((peers,)),
        ],
        compiler_params=pltpu.CompilerParams(
            collective_id=0, has_side_effects=True, vmem_limit_bytes=67043328
        ),
    )(
        heads_on.T,
        ffn_blocks.T,
        hidden_in.reshape(length, width),
        attn_gain,
        ffn_gain,
        *tables(length),
        w_query[0],
        w_key[0],
        w_value[0],
        w_out[0],
        w_gate[0],
        w_up[0],
        w_down[0],
    )
    return result.reshape(hidden_in.shape)


def one_device(*args):
    hidden_in, w_query, w_key, w_gate = args[0], args[2], args[3], args[7]
    sections, peers = lax.axis_size("section"), lax.axis_size("mp")
    fits = (
        hidden_in.shape[0] == 1
        and args[10].shape[0] == sections
        and peers == KV_HEADS
        and sections == 4
        and args[5].shape[1] == w_query.shape[2]
        and 2 * hidden_in.shape[2] == HD
        and w_query.shape[2] * KV_HEADS == HEADS * HD
        and w_key.shape[2] == HD
        and w_gate.shape[2] % TILE == 0
        and hidden_in.shape[3] % (peers * HD) == 0
        and hidden_in.shape[3] == HEADS * HD
    )
    return (resident if fits else per_device)(*args)


def solution(mesh):
    return jax.shard_map(
        one_device,
        mesh=mesh,
        in_specs=(
            P(None, "section", None, None),
            P("section", None),
            P("section", None, "mp"),
            P("section", None, "mp"),
            P("section", None, "mp"),
            P("section", "mp", None),
            P("section", None),
            P("section", None, "mp"),
            P("section", None, "mp"),
            P("section", "mp", None),
            P(None, "section"),
            P(None, "section"),
        ),
        out_specs=P(None, "section", None, None),
        check_vma=False,
    )
```
